32 devices in a mesh: ccy: 4 (over x, core), path: 8 (over z, y).
Axes of the slice: x: 2, y: 2, z: 4, core: 2. Of those that a mesh axis runs over, the one named last changes fastest.
Arguments:
- curve_store: bfloat16 [4, 16, 64, 2048], P('ccy', 'path'), may hold values from -0.13 to 0.18
- cash_index: int32 [4, 2048, 16], P('ccy'), may hold values from 0 to 1023
- cash_amount: float32 [4, 2048, 16], P('ccy'), may hold values from -0.6 to 0.6
- trade_set: int32 [4, 2048], P('ccy'), may hold values from 0 to 511
- date_slot: int32 [16], replicated, may hold values from 0 to 15, as said below
- default_weight: float32 [16, 512], replicated, may hold values from 0.02 to 0.2
Outputs:
- exposure: float32 [16, 512], P(None, 'ccy')
- node_sens: float32 [4, 16, 64], P('ccy')
The draws below stay inside these ranges and needn't reach their ends.
Inputs may be any that keep to these rules, and one draw needn't show every extreme that they name: `date_slot`: the 16 slots are distinct; slot s is stored at path index s // 2, position s % 2.
All inputs are finite; a program needn't handle non-finite values.
Results may differ from the reference program's by a relative error of at most 0.0029.
Values may be sent and summed in bfloat16 or wider, within the bound.
A program may use at most 64 MiB of HBM per device.

```python
import math
import jax
import jax.numpy as jnp
from jax import lax

NODES = 64
CFG = 1024
NSETS = 512
TRADES = 2048
NCF = 16
DATES = 16
PATHS = 2048
SLOTS_ALL = 16
N_CCY = 4


def draw_date_slot(key, part):
    return jax.random.permutation(key, SLOTS_ALL)[:DATES].astype(jnp.int32)


def draw_curve_store(key, part):
    level_key, spread_key, height_key, flip_key = jax.random.split(jax.random.fold_in(key, 7), 4)
    block_shape = (N_CCY, SLOTS_ALL, 1, PATHS)
    base_level = jax.random.uniform(level_key, block_shape, jnp.float32, 0.0, 0.05)
    jump_scale = jnp.exp(jax.random.uniform(spread_key, block_shape, jnp.float32, math.log(0.01), math.log(0.12)))
    jump_height = jax.random.uniform(height_key, (N_CCY, SLOTS_ALL, NODES, PATHS), jnp.float32, 0.5, 1.0)
    flip_bits = jax.random.randint(flip_key, block_shape, 0, 2)
    node_index = jnp.arange(NODES, dtype=jnp.int32).reshape(1, 1, NODES, 1)
    parity = (node_index + flip_bits) % 2
    signed = 1.0 - 2.0 * parity.astype(jnp.float32)
    return (base_level + jump_scale * signed * jump_height).astype(jnp.bfloat16)


def touch_ends(drawn, key, least, largest):
    spot = [jax.random.randint(jax.random.fold_in(key, axis), (), 0, length) for axis, length in enumerate(drawn.shape)]
    main_axis = drawn.shape.index(max(drawn.shape))
    neighbour = spot[:main_axis] + [(spot[main_axis] + 1) % drawn.shape[main_axis]] + spot[main_axis + 1:]
    return drawn.at[tuple(spot)].set(least).at[tuple(neighbour)].set(largest)


def level_of(own_key, dims, shards, least, top_value):
    def one(dim, blocks):
        draws = jax.random.uniform(jax.random.fold_in(jax.random.fold_in(own_key, 6), dim), (blocks,), jnp.float32, least / len(shards), top_value / len(shards))
        return jnp.repeat(jnp.exp(draws), dims[dim] // blocks).reshape((-1,) + (1,) * (len(dims) - dim - 1))

    gain = one(*shards[0])
    for cut in shards[1:]:
        gain = gain * one(*cut)
    return gain


def noise(stream_key, extent, scale, most, shards=(), held_as=jnp.bfloat16):
    entries = jax.random.normal(stream_key, extent, jnp.float32) * scale
    if len(shards) > 0:
        entries = level_of(stream_key, extent, shards, -0.22, 0.18) * entries
    return jnp.clip(entries, min=-most, max=most).astype(held_as)


def setup_inputs(seed: int = 0) -> dict:
    key_list = jax.random.split(jax.random.key(seed), 7)
    return {
        "curve_store": draw_curve_store(jax.random.fold_in(key_list[6], 71), 0),
        "cash_index": touch_ends(jax.random.randint(key_list[1], (N_CCY, TRADES, NCF), 0, CFG), jax.random.fold_in(key_list[1], 1), 0, CFG - 1).astype(jnp.int32),
        "cash_amount": noise(key_list[2], (N_CCY, TRADES, NCF), 0.1, 0.6, ((0, 4),), jnp.float32),
        "trade_set": touch_ends(jax.random.randint(key_list[3], (N_CCY, TRADES), 0, NSETS), jax.random.fold_in(key_list[3], 1), 0, NSETS - 1).astype(jnp.int32),
        "date_slot": draw_date_slot(jax.random.fold_in(key_list[6], 71), 0),
        "default_weight": jnp.clip(jnp.exp(jax.random.uniform(key_list[5], (DATES, NSETS), jnp.float32, math.log(0.02), math.log(0.2))), 0.02, 0.2),
    }


SOFTEN = 0.04
HORIZON = 32.0

def date_tables(date_index, node_count, grid_count):
    start_time = 0.5 * (jnp.asarray(date_index).astype(jnp.float32) + 1.0)
    grid_times = HORIZON * (jnp.arange(grid_count, dtype=jnp.float32) + 1.0) / grid_count
    tenors = HORIZON * (jnp.arange(node_count, dtype=jnp.float32) + 1.0) / node_count
    remain = grid_times - start_time
    alive_mask = (remain > 0.0).astype(jnp.float32)
    clipped = jnp.clip(remain, HORIZON / node_count, HORIZON)
    weights = jnp.maximum(0.0, 1.0 - jnp.abs(clipped[None, :] - tenors[:, None]) * (node_count / HORIZON))
    return (remain, alive_mask, weights)

def netted_cash(flow_index, amount, trade_sets):
    columns = jnp.repeat(trade_sets, flow_index.shape[1]).astype(jnp.int32)
    cash_table = jnp.zeros((CFG, NSETS), jnp.float32).at[flow_index.reshape(-1).astype(jnp.int32), columns].add(amount.reshape(-1).astype(jnp.float32))
    return cash_table.astype(jnp.bfloat16)

def reference(curve_store, cash_index, cash_amount, trade_set, date_slot, default_weight):
    total_paths = curve_store.shape[3]
    tables = [netted_cash(cash_index[member], cash_amount[member], trade_set[member]) for member in range(N_CCY)]
    exposure_rows = []
    sens_rows = []
    for date_index in range(DATES):
        remain, alive_mask, weights = date_tables(date_index, NODES, CFG)
        grid_weights = weights.astype(jnp.bfloat16)
        values = jnp.zeros((total_paths, NSETS), jnp.float32)
        discounts = []
        for member in range(N_CCY):
            curve_now = lax.dynamic_index_in_dim(curve_store[member], date_slot[date_index].astype(jnp.int32), 0, keepdims=False)
            yields = lax.dot_general(curve_now, grid_weights, (((0,), (0,)), ((), ())), preferred_element_type=jnp.float32)
            discount = alive_mask * jnp.exp(-yields * remain)
            discounts.append(discount)
            values = values + jnp.dot(discount.astype(jnp.bfloat16), tables[member], preferred_element_type=jnp.float32)
        rooted = jnp.sqrt(values * values + SOFTEN)
        exposure_rows.append(lax.optimization_barrier(jnp.sum(0.5 * (values + rooted), axis=0)) / total_paths)
        slopes = (default_weight[date_index] / total_paths * 0.5 * (1.0 + values / rooted)).astype(jnp.bfloat16)
        group_sens = []
        for member in range(N_CCY):
            back_flow = lax.dot_general(slopes, tables[member], (((1,), (1,)), ((), ())), preferred_element_type=jnp.float32)
            node_pull = lax.optimization_barrier(jnp.sum(back_flow * -remain * discounts[member], axis=0))
            group_sens.append(jnp.dot(weights, node_pull, precision=lax.Precision.HIGHEST))
        sens_rows.append(jnp.stack(group_sens))
    return (jnp.stack(exposure_rows), jnp.stack(sens_rows, axis=1))
```

```python
import functools

import jax
import jax.numpy as jnp
from jax import lax
from jax.experimental import pallas as pl
from jax.experimental.pallas import tpu as pltpu
from jax.sharding import PartitionSpec as P

NSETS = 512
CFG = 1024
SOFTEN = 0.04
HORIZON = 32.0
LOG2E = 1.4426950408889634


def date_tables(date_index, node_count, grid_count):
    start_time = 0.5 * (jnp.asarray(date_index).astype(jnp.float32) + 1.0)
    grid_times = HORIZON * (jnp.arange(grid_count, dtype=jnp.float32) + 1.0) / grid_count
    tenors = HORIZON * (jnp.arange(node_count, dtype=jnp.float32) + 1.0) / node_count
    remain = grid_times - start_time
    alive_mask = (remain > 0.0).astype(jnp.float32)
    clipped = jnp.clip(remain, HORIZON / node_count, HORIZON)
    weights = jnp.maximum(
        0.0, 1.0 - jnp.abs(clipped[None, :] - tenors[:, None]) * (node_count / HORIZON)
    )
    return (remain, alive_mask, weights)


def cash_kernel(rows, base_ref, index_ref, amount_ref, set_ref, out_ref, a_hi, a_lo):
    flows, trades = index_ref.shape
    nsets = out_ref.shape[1]
    wanted = lax.broadcasted_iota(jnp.int32, (rows, 128), 0) + base_ref[0]

    @pl.loop(0, trades // 128)
    def _(tile):
        cols = pl.ds(pl.multiple_of(tile * 128, 128), 128)
        total = jnp.zeros((rows, 128), jnp.float32)
        index = index_ref[:, cols]
        amount = amount_ref[:, cols]
        for k in range(flows):
            hit = wanted == index[k : k + 1, :]
            total = total + jnp.where(hit, amount[k : k + 1, :], 0.0)
        high = total.astype(jnp.bfloat16)
        a_hi[:, cols] = high
        a_lo[:, cols] = (total - high.astype(jnp.float32)).astype(jnp.bfloat16)

    sets = lax.broadcasted_iota(jnp.int32, (nsets, trades), 0)
    onehot = jnp.where(sets == set_ref[...], 1.0, 0.0).astype(jnp.bfloat16)
    dims = (((1,), (1,)), ((), ()))
    table = lax.dot_general(a_hi[...], onehot, dims, preferred_element_type=jnp.float32)
    table = table + lax.dot_general(a_lo[...], onehot, dims, preferred_element_type=jnp.float32)
    out_ref[...] = table.astype(jnp.bfloat16)


def build_cash(base, flow_index, amount, trade_sets, rows, nsets):
    flows, trades = flow_index.shape[1], flow_index.shape[0]
    vmem = pl.BlockSpec(memory_space=pltpu.VMEM)
    return pl.pallas_call(
        functools.partial(cash_kernel, rows),
        out_shape=jax.ShapeDtypeStruct((rows, nsets), jnp.bfloat16),
        in_specs=[pl.BlockSpec(memory_space=pltpu.SMEM), vmem, vmem, vmem],
        out_specs=vmem,
        scratch_shapes=[pltpu.VMEM((rows, trades), jnp.bfloat16)] * 2,
        cost_estimate=pl.CostEstimate(
            flops=4 * rows * trades * nsets, bytes_accessed=4 * trades * flows, transcendentals=0
        ),
        name="cash_rows",
    )(base, flow_index.T, amount.T, trade_sets[None, :])


def fused_kernel(
    total_paths, date_ref, index_ref, amount_ref, set_ref, weight_ref, curve_ref, exp_ref, sens_ref,
    table, onehot, cash, other, curves, knots, coef, grid, column, disc, value, slope, part, held,
    send, recv, own,
):
    groups, slots, nodes, paths = curves.shape
    flows, trades = index_ref.shape
    cfg, half = cash.shape[1], cash.shape[2]
    nsets = 2 * half
    members = held.shape[1]
    levels = members // 2
    rows = cfg // members
    dates = date_ref.shape[0]
    per = cfg // nodes
    step = HORIZON / cfg
    c, p = lax.axis_index("ccy"), lax.axis_index("path")
    x, k = c // 2, c % 2
    z, y = p // 2, p % 2
    sibling = c + 1 - 2 * k
    across = (c + 2) % groups
    diagonal = (sibling + 2) % groups
    beside = p + 1 - 2 * y
    barrier = pltpu.get_barrier_semaphore()
    targets = [
        ((c + dc) % groups, (p + dp) % members) for dc in range(groups) for dp in range(members)
    ][1:]
    for target in targets:
        pl.semaphore_signal(barrier, inc=1, device_id=target, device_id_type=pl.DeviceIdType.MESH)

    started = []

    def remote(source, target, device):
        n = len(started)
        copy = pltpu.make_async_remote_copy(
            src_ref=source, dst_ref=target, send_sem=send.at[n], recv_sem=recv.at[n],
            device_id=device, device_id_type=pl.DeviceIdType.MESH,
        )
        copy.start()
        started.append(copy)
        return copy

    def lanes(which):
        return pl.ds(pl.multiple_of(which * paths, 128), paths)

    keep = pltpu.make_async_copy(curve_ref.at[:, :, lanes(k)], curves.at[c], own.at[0])
    keep.start()

    def block(g, level, side):
        at = (side * levels + level) * rows
        return cash.at[g, pl.ds(pl.multiple_of(at, 16), rows), :]

    wanted = lax.broadcasted_iota(jnp.int32, (rows, 128), 0) + (y * levels + z) * rows
    sets = lax.broadcasted_iota(jnp.int32, (nsets, 128), 0)

    @pl.loop(0, trades // 128)
    def _(tile):
        cols = pl.ds(pl.multiple_of(tile * 128, 128), 128)
        total = jnp.zeros((rows, 128), jnp.float32)
        index = index_ref[:, cols]
        amount = amount_ref[:, cols]
        for n in range(flows):
            hit = wanted == index[n : n + 1, :]
            total = total + jnp.where(hit, amount[n : n + 1, :], 0.0)
        high = total.astype(jnp.bfloat16)
        table[0:rows, cols] = high
        table[rows : 2 * rows, cols] = (total - high.astype(jnp.float32)).astype(jnp.bfloat16)
        onehot[:, cols] = jnp.where(sets == set_ref[:, cols], 1.0, 0.0).astype(jnp.bfloat16)

    both = lax.dot_general(
        onehot[...], table[...], (((1,), (1,)), ((), ())), preferred_element_type=jnp.float32
    )
    netted = jnp.transpose(both[:, :rows] + both[:, rows:]).astype(jnp.bfloat16)
    here = pl.ds(pl.multiple_of((y * levels + z) * rows, 16), rows)
    low, top = netted[:, :half], netted[:, half:]
    cash[c, here, :] = jnp.where(x == 0, low, top)
    other[...] = jnp.where(x == 0, top, low)

    pl.semaphore_wait(barrier, len(targets))
    near, core, over = (c, beside), (sibling, p), (across, p)
    mine = block(c, z, y)
    crossing = remote(other, mine, over)
    up = [(n, remote(mine, mine, (c, ((z + n) % levels) * 2 + y))) for n in range(1, levels)]
    sides = [[(z, remote(mine, mine, near))], []]
    given = [[remote(mine, mine, core)], [], [], []]
    arriving = {}
    for s in range(slots):
        arriving["sibling", s] = remote(curve_ref.at[s, :, lanes(1 - k)], curves.at[c, s], core)
    for s in range(slots):
        arriving["across", s] = remote(curve_ref.at[s, :, lanes(k)], curves.at[c, s], over)
        arriving["diagonal", s] = remote(curve_ref.at[s, :, lanes(1 - k)], curves.at[c, s], (diagonal, p))

    starts = []
    for s in range(slots):
        date = jnp.int32(0)
        for d in range(dates):
            date = date + jnp.where(date_ref[d] == p * slots + s, d, 0)
        shift = (date + 1).astype(jnp.float32)
        starts.append((date, shift))
        at = lax.broadcasted_iota(jnp.int32, (cfg, 128), 0).astype(jnp.float32)
        whole = at + 1.0 - shift * per
        place = lax.broadcasted_iota(jnp.int32, (cfg, 128), 0) % per
        part_up = (place.astype(jnp.float32) + 1.0) * (1.0 / per)
        scaled = whole * (-LOG2E * step)
        live = whole > 0.0
        coef[s, 0] = jnp.where(live, scaled * (1.0 - part_up), -1000.0)
        coef[s, 1] = jnp.where(live, scaled * part_up, 0.0)
        coef[s, 2] = whole * -step
        flat = lax.broadcasted_iota(jnp.int32, (nodes, cfg), 1).astype(jnp.float32)
        left = jnp.clip((flat + 1.0) * step - shift * (HORIZON / nodes), HORIZON / nodes, HORIZON)
        tenors = (lax.broadcasted_iota(jnp.int32, (nodes, cfg), 0).astype(jnp.float32) + 1.0) * (HORIZON / nodes)
        grid[s] = jnp.maximum(0.0, 1.0 - jnp.abs(left - tenors) * (nodes / HORIZON)).astype(jnp.bfloat16)
        line = lax.broadcasted_iota(jnp.int32, (dates, half), 0) == date
        row = jnp.where(x == 0, weight_ref[:, :half], weight_ref[:, half:])
        row = jnp.sum(jnp.where(line, row, 0.0), axis=0, keepdims=True) / total_paths * 0.5
        column[s] = jnp.transpose(jnp.broadcast_to(row, (128, half)))

    def discount(g, s):
        extent = knots.shape[0]
        shift = starts[s][1]
        node = lax.broadcasted_iota(jnp.int32, (extent, nodes), 0).astype(jnp.float32) - shift - 1.0
        node = jnp.where(node == -1.0, 0.0, node)
        pick = node == lax.broadcasted_iota(jnp.int32, (extent, nodes), 1).astype(jnp.float32)
        pick = jnp.where(pick, 1.0, 0.0).astype(jnp.bfloat16)
        moved = jnp.dot(pick, curves[g, s], preferred_element_type=jnp.float32)
        node = lax.broadcasted_iota(jnp.int32, (extent, 1), 0).astype(jnp.float32) - shift - 1.0
        knots[...] = moved + jnp.where(node < -1.5, 1.0, 0.0)

        @pl.loop(0, nodes // 8)
        def _(i):
            base = pl.multiple_of(i * 8 * per, 8 * per)
            target = pl.multiple_of(g * cfg + i * 8 * per, 8 * per)
            first = pl.multiple_of(i * 8, 8)
            for tile in range(paths // 128):
                cols = slice(tile * 128, tile * 128 + 128)
                below = knots[pl.ds(first, 8), cols]
                after = knots[pl.ds(first + 8, 8), cols]
                for n in range(8):
                    down = coef[s, 0, pl.ds(base + n * per, per), :]
                    above = coef[s, 1, pl.ds(base + n * per, per), :]
                    upper = below[n + 1 : n + 2] if n < 7 else after[0:1]
                    power = down * below[n : n + 1] + above * upper
                    disc[s, pl.ds(target + n * per, per), cols] = jnp.exp2(power).astype(jnp.bfloat16)

    stretch = cfg // 2
    fresh = [True] * slots

    def accumulate(g, side, s):
        at = pl.ds(pl.multiple_of(side * stretch, 16), stretch)
        down = pl.ds(pl.multiple_of(g * cfg + side * stretch, 16), stretch)
        product = lax.dot_general(
            cash[g, at, :], disc[s, down, :], (((0,), (0,)), ((), ())), preferred_element_type=jnp.float32
        )
        if fresh[s]:
            value[s] = product
        else:
            value[s] = value[s] + product
        fresh[s] = False

    keep.wait()
    discount(c, 0)
    crossing.wait_recv()
    got = block(across, z, y)
    upper = [(n, remote(got, got, (c, ((z + n) % levels) * 2 + y))) for n in range(1, levels)]
    sides[1].append((z, remote(got, got, near)))
    given[1].append(remote(got, got, core))
    for s in range(1, slots):
        discount(c, s)
    for which, g, copies in ((0, c, up), (1, across, upper)):
        for n, copy in copies:
            copy.wait_recv()
            level = (z - n + levels) % levels
            there = block(g, level, y)
            sides[which].append((level, remote(there, there, near)))
            given[which].append(remote(there, there, core))
        if which == 0:
            for s in range(slots):
                arriving["sibling", s].wait_recv()
                discount(sibling, s)
            for s in range(slots):
                accumulate(c, y, s)
    for which, g in ((0, c), (1, across)):
        if which == 0:
            for name, h in (("across", across), ("diagonal", diagonal)):
                arriving[name, 0].wait_recv()
                discount(h, 0)
                accumulate(across, y, 0) if name == "across" else None
            for copy in given[0] + given[1]:
                copy.wait_recv()
            for s in range(slots):
                accumulate(sibling, y, s)
        for level, copy in sides[which]:
            copy.wait_recv()
            there = block(g, level, 1 - y)
            given[2 + which].append(remote(there, there, core))
        if which == 0:
            for s in range(slots):
                accumulate(c, 1 - y, s)
            for s in range(1, slots):
                for name, h in (("across", across), ("diagonal", diagonal)):
                    arriving[name, s].wait_recv()
                    discount(h, s)
                accumulate(across, y, s)
            for s in range(slots):
                accumulate(diagonal, y, s)
    for s in range(slots):
        accumulate(across, 1 - y, s)
    for which, g in ((2, sibling), (3, diagonal)):
        for copy in given[which]:
            copy.wait_recv()
        for s in range(slots):
            accumulate(g, 1 - y, s)

    part[...] = jnp.zeros(part.shape, jnp.float32)
    for s in range(slots):
        gained = jnp.zeros((half, 128), jnp.float32)
        for tile in range(paths // 128):
            cols = slice(tile * 128, tile * 128 + 128)
            held_value = value[s, :, cols]
            square = held_value * held_value + SOFTEN
            inverse = lax.rsqrt(square)
            gained = gained + 0.5 * (held_value + square * inverse)
            steep = column[s] * (1.0 + held_value * inverse)
            slope[s, cols, :] = jnp.transpose(steep).astype(jnp.bfloat16)
        gained = jnp.sum(jnp.transpose(gained), axis=0, keepdims=True) / total_paths
        for n in range(2):
            part[2 * x + n, s : s + 1, :] = gained[:, n * 128 : n * 128 + 128]

    for s in range(slots):
        for g in range(groups):
            down = pl.ds(g * cfg, cfg)
            pulled = jnp.dot(disc[s, down, :], slope[s], preferred_element_type=jnp.float32)
            pulled = pulled * cash[g].astype(jnp.float32)
            summed = (pulled[:, :128] + pulled[:, 128:]) * coef[s, 2]
            high = summed.astype(jnp.bfloat16)
            rest = (summed - high.astype(jnp.float32)).astype(jnp.bfloat16)
            pair = jnp.dot(
                grid[s], jnp.concatenate([high, rest], axis=1), preferred_element_type=jnp.float32
            )
            spread = jnp.transpose(pair[:, :128] + pair[:, 128:])
            part[g, slots + s : slots + s + 1, :nodes] = jnp.sum(spread, axis=0, keepdims=True)

    sums = [remote(part.at[g], held.at[c, p], (g, q)) for g, q in targets]
    held[c, p] = part[c]
    for copy in sums:
        copy.wait_recv()
    for d in range(dates):
        slot = date_ref[d]
        q = slot // slots
        s = slot % slots
        gains = held[2 * x, q] + held[2 * x + 1, q]
        total = held[0, q]
        for g in range(1, groups):
            total = total + held[g, q]
        gain, sens = gains[0:1], total[slots : slots + 1]
        for n in range(1, slots):
            gain = jnp.where(s == n, gains[n : n + 1], gain)
            sens = jnp.where(s == n, total[slots + n : slots + n + 1], sens)
        exp_ref[d : d + 1, :] = gain
        sens_ref[d : d + 1, :] = sens[:, :nodes]
    for copy in started:
        copy.wait_send()


def by_slot(curve_store, cash_index, cash_amount, trade_set, date_slot, default_weight):
    groups, members = lax.axis_size("ccy"), lax.axis_size("path")
    _, slots, nodes, total_paths = curve_store.shape
    trades, flows = cash_index.shape[1:]
    dates, nsets = default_weight.shape
    rows, half, paths = CFG // members, nsets // 2, total_paths // 2
    levels = members // 2
    parts = -(-2 * slots // 8) * 8
    count = 1 + 2 * (levels - 1) + 2 * levels + 4 * levels + 3 * slots + groups * members - 1
    smem = pl.BlockSpec(memory_space=pltpu.SMEM)
    vmem = pl.BlockSpec(memory_space=pltpu.VMEM)
    bf16, f32 = jnp.bfloat16, jnp.float32
    exposure, sens = pl.pallas_call(
        functools.partial(fused_kernel, total_paths),
        out_shape=[
            jax.ShapeDtypeStruct((dates, nsets // groups), f32),
            jax.ShapeDtypeStruct((dates, nodes), f32),
        ],
        in_specs=[smem, vmem, vmem, vmem, vmem, pl.BlockSpec(memory_space=pl.ANY)],
        out_specs=[vmem, vmem],
        scratch_shapes=[
            pltpu.VMEM((2 * rows, trades), bf16),
            pltpu.VMEM((nsets, trades), bf16),
            pltpu.VMEM((groups, CFG, half), bf16),
            pltpu.VMEM((rows, half), bf16),
            pltpu.VMEM((groups, slots, nodes, paths), bf16),
            pltpu.VMEM((nodes + 8, paths), f32),
            pltpu.VMEM((slots, 3, CFG, 128), f32),
            pltpu.VMEM((slots, nodes, CFG), bf16),
            pltpu.VMEM((slots, half, 128), f32),
            pltpu.VMEM((slots, groups * CFG, paths), bf16),
            pltpu.VMEM((slots, half, paths), f32),
            pltpu.VMEM((slots, paths, half), bf16),
            pltpu.VMEM((groups, parts, 128), f32),
            pltpu.VMEM((groups, members, parts, 128), f32),
            pltpu.SemaphoreType.DMA((count,)),
            pltpu.SemaphoreType.DMA((count,)),
            pltpu.SemaphoreType.DMA((1,)),
        ],
        compiler_params=pltpu.CompilerParams(collective_id=0, has_side_effects=True),
        name="fused",
    )(date_slot, cash_index[0].T, cash_amount[0].T, trade_set, default_weight, curve_store[0])
    return (exposure, sens[None])


def by_path(curve_store, cash_index, cash_amount, trade_set, date_slot, default_weight):
    groups = lax.axis_size("ccy")
    group_index = lax.axis_index("ccy")
    members = lax.axis_size("path")
    nodes, total_paths = curve_store.shape[2], curve_store.shape[3]
    nsets = default_weight.shape[1]
    share_size = nsets // groups
    rows = CFG // members
    base = (lax.axis_index("path") * rows).astype(jnp.int32)[None]
    chunk = build_cash(base, cash_index[0], cash_amount[0], trade_set[0], rows, nsets)
    cash_table = lax.all_gather(chunk, "path", axis=0, tiled=True)
    blocks = lax.all_to_all(curve_store, "path", split_axis=3, concat_axis=1, tiled=True)[0]
    cash_all = lax.all_gather(cash_table[None], "ccy", axis=0, tiled=True)

    def advance(unused, inputs):
        date_index, slot_id, weight_row = inputs
        remain, alive_mask, weights = date_tables(date_index, nodes, CFG)
        grid_weights = weights.astype(jnp.bfloat16)
        curve_now = lax.dynamic_index_in_dim(blocks, slot_id, 0, keepdims=False)
        curve_groups = lax.all_gather(curve_now[None], "ccy", axis=0, tiled=True)
        yields = jnp.einsum(
            "gnp,nc->gpc", curve_groups, grid_weights, preferred_element_type=jnp.float32
        )
        discount_all = alive_mask * jnp.exp(-yields * remain)
        values = jnp.einsum(
            "gpc,gcs->ps", discount_all.astype(jnp.bfloat16), cash_all,
            preferred_element_type=jnp.float32,
        )
        discount = lax.dynamic_index_in_dim(discount_all, group_index, 0, keepdims=False)
        rooted = jnp.sqrt(values * values + SOFTEN)
        slopes = (weight_row / total_paths * 0.5 * (1.0 + values / rooted)).astype(jnp.bfloat16)
        share_values = lax.dynamic_slice_in_dim(values, group_index * share_size, share_size, 1)
        share_root = lax.dynamic_slice_in_dim(rooted, group_index * share_size, share_size, 1)
        exposure_part = jnp.sum(0.5 * (share_values + share_root), axis=0) / total_paths
        back_flow = lax.dot_general(
            slopes, cash_table, (((1,), (1,)), ((), ())), preferred_element_type=jnp.float32
        )
        node_pull = jnp.sum(back_flow * -remain * discount, axis=0)
        sens_part = jnp.dot(weights, node_pull, precision=lax.Precision.HIGHEST)
        exposure_part, sens_part = lax.psum((exposure_part, sens_part), "path")
        return (unused, (exposure_part, sens_part))

    inputs = (jnp.arange(date_slot.shape[0], dtype=jnp.int32), date_slot, default_weight)
    _, (exposure_rows, sens_rows) = lax.scan(advance, jnp.zeros((), jnp.float32), inputs)
    return (exposure_rows, sens_rows[None])


def local(curve_store, cash_index, cash_amount, trade_set, date_slot, default_weight):
    groups, members = lax.axis_size("ccy"), lax.axis_size("path")
    slots, nodes, total_paths = curve_store.shape[1:]
    nsets = default_weight.shape[1]
    trades = trade_set.shape[1]
    fits = groups == 4 and members % 2 == 0 and slots * members == date_slot.shape[0]
    fits = fits and nodes * 0.5 == HORIZON and CFG == 16 * nodes and total_paths % 256 == 0
    fits = fits and nsets == 4 * 128 and CFG // members == 128 and trades % 128 == 0
    plan = by_slot if fits else by_path
    return plan(curve_store, cash_index, cash_amount, trade_set, date_slot, default_weight)


def solution(mesh):
    in_specs = (
        P("ccy", "path", None, None),
        P("ccy", None, None),
        P("ccy", None, None),
        P("ccy", None),
        P(),
        P(),
    )
    out_specs = (P(None, "ccy"), P("ccy", None, None))
    return jax.shard_map(local, mesh=mesh, in_specs=in_specs, out_specs=out_specs, check_vma=False)
```

```python
import functools

import jax
import jax.numpy as jnp
from jax import lax
from jax.experimental import pallas as pl
from jax.experimental.pallas import tpu as pltpu
from jax.sharding import PartitionSpec as P

NSETS = 512
CFG = 1024
SOFTEN = 0.04
HORIZON = 32.0
LOG2E = 1.4426950408889634


def date_tables(date_index, node_count, grid_count):
    start_time = 0.5 * (jnp.asarray(date_index).astype(jnp.float32) + 1.0)
    grid_times = HORIZON * (jnp.arange(grid_count, dtype=jnp.float32) + 1.0) / grid_count
    tenors = HORIZON * (jnp.arange(node_count, dtype=jnp.float32) + 1.0) / node_count
    remain = grid_times - start_time
    alive_mask = (remain > 0.0).astype(jnp.float32)
    clipped = jnp.clip(remain, HORIZON / node_count, HORIZON)
    weights = jnp.maximum(
        0.0, 1.0 - jnp.abs(clipped[None, :] - tenors[:, None]) * (node_count / HORIZON)
    )
    return (remain, alive_mask, weights)


def cash_kernel(rows, base_ref, index_ref, amount_ref, set_ref, out_ref, a_hi, a_lo):
    flows, trades = index_ref.shape
    nsets = out_ref.shape[1]
    wanted = lax.broadcasted_iota(jnp.int32, (rows, 128), 0) + base_ref[0]

    @pl.loop(0, trades // 128)
    def _(tile):
        cols = pl.ds(pl.multiple_of(tile * 128, 128), 128)
        total = jnp.zeros((rows, 128), jnp.float32)
        index = index_ref[:, cols]
        amount = amount_ref[:, cols]
        for k in range(flows):
            hit = wanted == index[k : k + 1, :]
            total = total + jnp.where(hit, amount[k : k + 1, :], 0.0)
        high = total.astype(jnp.bfloat16)
        a_hi[:, cols] = high
        a_lo[:, cols] = (total - high.astype(jnp.float32)).astype(jnp.bfloat16)

    sets = lax.broadcasted_iota(jnp.int32, (nsets, trades), 0)
    onehot = jnp.where(sets == set_ref[...], 1.0, 0.0).astype(jnp.bfloat16)
    dims = (((1,), (1,)), ((), ()))
    table = lax.dot_general(a_hi[...], onehot, dims, preferred_element_type=jnp.float32)
    table = table + lax.dot_general(a_lo[...], onehot, dims, preferred_element_type=jnp.float32)
    out_ref[...] = table.astype(jnp.bfloat16)


def build_cash(base, flow_index, amount, trade_sets, rows, nsets):
    flows, trades = flow_index.shape[1], flow_index.shape[0]
    vmem = pl.BlockSpec(memory_space=pltpu.VMEM)
    return pl.pallas_call(
        functools.partial(cash_kernel, rows),
        out_shape=jax.ShapeDtypeStruct((rows, nsets), jnp.bfloat16),
        in_specs=[pl.BlockSpec(memory_space=pltpu.SMEM), vmem, vmem, vmem],
        out_specs=vmem,
        scratch_shapes=[pltpu.VMEM((rows, trades), jnp.bfloat16)] * 2,
        cost_estimate=pl.CostEstimate(
            flops=4 * rows * trades * nsets, bytes_accessed=4 * trades * flows, transcendentals=0
        ),
        name="cash_rows",
    )(base, flow_index.T, amount.T, trade_sets[None, :])


def fused_kernel(
    total_paths, date_ref, index_hbm, amount_hbm, set_hbm, weight_hbm, curve_ref, exp_ref, sens_ref,
    index_ref, amount_ref, set_ref, weight_ref, table, onehot, cash, other, curves, coef, pull, grid,
    column, disc, value, slope, summed, part, held, send, recv, own,
):
    groups, slots, nodes, paths = curves.shape
    flows, trades = index_ref.shape
    cfg, half = cash.shape[1], cash.shape[2]
    nsets = 2 * half
    members = held.shape[1]
    levels = members // 2
    rows = cfg // members
    dates = date_ref.shape[0]
    per = cfg // nodes
    step = HORIZON / cfg
    c, p = lax.axis_index("ccy"), lax.axis_index("path")
    x, k = c // 2, c % 2
    z, y = p // 2, p % 2
    sibling = c + 1 - 2 * k
    across = (c + 2) % groups
    diagonal = (sibling + 2) % groups
    beside = p + 1 - 2 * y
    barrier = pltpu.get_barrier_semaphore()
    others = [
        ((c + dc) % groups, (p + dp) % members) for dc in range(groups) for dp in range(members)
    ][1:]
    peers = [(sibling, p), (across, p), (diagonal, p), (c, beside)]
    peers += [(c, ((z + n) % levels) * 2 + y) for n in range(1, levels)]
    for peer in peers:
        pl.semaphore_signal(barrier, inc=1, device_id=peer, device_id_type=pl.DeviceIdType.MESH)
    loads = [
        pltpu.make_async_copy(source, target, own.at[1 + n])
        for n, (source, target) in enumerate(
            ((index_hbm, index_ref), (amount_hbm, amount_ref), (set_hbm, set_ref), (weight_hbm, weight_ref))
        )
    ]
    for load in loads:
        load.start()

    started = []

    def remote(source, target, device):
        n = len(started)
        copy = pltpu.make_async_remote_copy(
            src_ref=source, dst_ref=target, send_sem=send.at[n], recv_sem=recv.at[n],
            device_id=device, device_id_type=pl.DeviceIdType.MESH,
        )
        copy.start()
        started.append(copy)
        return copy

    def lanes(which):
        return pl.ds(pl.multiple_of(which * paths, 128), paths)

    keep = pltpu.make_async_copy(curve_ref.at[:, :, lanes(k)], curves.at[c], own.at[0])
    keep.start()

    def block(g, level, side):
        at = (side * levels + level) * rows
        return cash.at[g, pl.ds(pl.multiple_of(at, 16), rows), :]

    wanted = lax.broadcasted_iota(jnp.int32, (rows, 128), 0) + (y * levels + z) * rows
    sets = lax.broadcasted_iota(jnp.int32, (nsets, 128), 0)
    for load in loads:
        load.wait()

    @pl.loop(0, trades // 128)
    def _(tile):
        cols = pl.ds(pl.multiple_of(tile * 128, 128), 128)
        total = jnp.zeros((rows, 128), jnp.float32)
        index = index_ref[:, cols]
        amount = amount_ref[:, cols]
        for n in range(flows):
            hit = wanted == index[n : n + 1, :]
            total = total + jnp.where(hit, amount[n : n + 1, :], 0.0)
        high = total.astype(jnp.bfloat16)
        table[0:rows, cols] = high
        table[rows : 2 * rows, cols] = (total - high.astype(jnp.float32)).astype(jnp.bfloat16)
        onehot[:, cols] = jnp.where(sets == set_ref[:, cols], 1.0, 0.0).astype(jnp.bfloat16)

    both = lax.dot_general(
        onehot[...], table[...], (((1,), (1,)), ((), ())), preferred_element_type=jnp.float32
    )
    netted = jnp.transpose(both[:, :rows] + both[:, rows:]).astype(jnp.bfloat16)
    here = pl.ds(pl.multiple_of((y * levels + z) * rows, 16), rows)
    low, top = netted[:, :half], netted[:, half:]
    cash[c, here, :] = jnp.where(x == 0, low, top)
    other[...] = jnp.where(x == 0, top, low)

    pl.semaphore_wait(barrier, len(peers))
    near, core, over = (c, beside), (sibling, p), (across, p)
    mine = block(c, z, y)
    crossing = remote(other, mine, over)
    up = [(n, remote(mine, mine, (c, ((z + n) % levels) * 2 + y))) for n in range(1, levels)]
    sides = [[(z, remote(mine, mine, near))], []]
    given = [[remote(mine, mine, core)], [], [], []]
    arriving = {}
    for s in range(slots):
        arriving["sibling", s] = remote(curve_ref.at[s, :, lanes(1 - k)], curves.at[c, s], core)
    for s in range(slots):
        arriving["across", s] = remote(curve_ref.at[s, :, lanes(k)], curves.at[c, s], over)
        arriving["diagonal", s] = remote(curve_ref.at[s, :, lanes(1 - k)], curves.at[c, s], (diagonal, p))

    starts = []
    for s in range(slots):
        date = jnp.int32(0)
        for d in range(dates):
            date = date + jnp.where(date_ref[d] == p * slots + s, d, 0)
        shift = (date + 1).astype(jnp.float32)
        starts.append((date, shift))
        at = lax.broadcasted_iota(jnp.int32, (cfg, nodes), 0).astype(jnp.float32)
        after = (at + 1.0) * step - shift * (HORIZON / nodes)
        inside = jnp.clip(after, HORIZON / nodes, HORIZON)
        tenor = (lax.broadcasted_iota(jnp.int32, (cfg, nodes), 1).astype(jnp.float32) + 1.0) * (HORIZON / nodes)
        weight = jnp.maximum(0.0, 1.0 - jnp.abs(inside - tenor) * (nodes / HORIZON))
        rest = jnp.where(after > 0.0, weight * (after * -LOG2E), 0.0)
        for n in range(3):
            piece = rest.astype(jnp.bfloat16)
            rest = rest - piece.astype(jnp.float32)
            coef[s, :, n * nodes : n * nodes + nodes] = piece
        first = lax.broadcasted_iota(jnp.int32, (cfg, nodes), 1) == 0
        dead = jnp.where(first, jnp.where(after > 0.0, 0.0, -1000.0), 0.0)
        coef[s, :, 3 * nodes : 4 * nodes] = dead.astype(jnp.bfloat16)
        at = lax.broadcasted_iota(jnp.int32, (cfg, 128), 0).astype(jnp.float32)
        pull[s] = shift * (HORIZON / nodes) - (at + 1.0) * step
        flat = lax.broadcasted_iota(jnp.int32, (nodes, cfg), 1).astype(jnp.float32)
        left = jnp.clip((flat + 1.0) * step - shift * (HORIZON / nodes), HORIZON / nodes, HORIZON)
        tenors = (lax.broadcasted_iota(jnp.int32, (nodes, cfg), 0).astype(jnp.float32) + 1.0) * (HORIZON / nodes)
        grid[s] = jnp.maximum(0.0, 1.0 - jnp.abs(left - tenors) * (nodes / HORIZON)).astype(jnp.bfloat16)
        line = lax.broadcasted_iota(jnp.int32, (dates, half), 0) == date
        row = jnp.where(x == 0, weight_ref[:, :half], weight_ref[:, half:])
        row = jnp.sum(jnp.where(line, row, 0.0), axis=0, keepdims=True) / total_paths * 0.5
        column[s] = jnp.transpose(jnp.broadcast_to(row, (128, half)))

    def discount(g, s):
        curve = curves[g, s]
        lines = jnp.concatenate([curve, curve, curve, jnp.ones(curve.shape, jnp.bfloat16)], axis=0)
        for m in range(0, cfg, 256):
            power = jnp.dot(coef[s, m : m + 256, :], lines, preferred_element_type=jnp.float32)
            target = pl.ds(pl.multiple_of(g * cfg + m, 256), 256)
            disc[s, target, :] = jnp.exp2(power).astype(jnp.bfloat16)

    stretch = cfg // 2
    fresh = [True] * slots

    def accumulate(g, side, s):
        at = pl.ds(pl.multiple_of(side * stretch, 16), stretch)
        down = pl.ds(pl.multiple_of(g * cfg + side * stretch, 16), stretch)
        product = lax.dot_general(
            cash[g, at, :], disc[s, down, :], (((0,), (0,)), ((), ())), preferred_element_type=jnp.float32
        )
        if fresh[s]:
            value[s] = product
        else:
            value[s] = value[s] + product
        fresh[s] = False

    keep.wait()
    discount(c, 0)
    crossing.wait_recv()
    got = block(across, z, y)
    upper = [(n, remote(got, got, (c, ((z + n) % levels) * 2 + y))) for n in range(1, levels)]
    sides[1].append((z, remote(got, got, near)))
    given[1].append(remote(got, got, core))
    for s in range(1, slots):
        discount(c, s)
    for which, g, copies in ((0, c, up), (1, across, upper)):
        for n, copy in copies:
            copy.wait_recv()
            level = (z - n + levels) % levels
            there = block(g, level, y)
            sides[which].append((level, remote(there, there, near)))
            given[which].append(remote(there, there, core))
        if which == 0:
            for s in range(slots):
                arriving["sibling", s].wait_recv()
                discount(sibling, s)
            for s in range(slots):
                accumulate(c, y, s)
    for which, g in ((0, c), (1, across)):
        if which == 0:
            for name, h in (("across", across), ("diagonal", diagonal)):
                arriving[name, 0].wait_recv()
                discount(h, 0)
                accumulate(across, y, 0) if name == "across" else None
            for copy in given[0] + given[1]:
                copy.wait_recv()
            for s in range(slots):
                accumulate(sibling, y, s)
        for level, copy in sides[which]:
            copy.wait_recv()
            there = block(g, level, 1 - y)
            given[2 + which].append(remote(there, there, core))
        if which == 0:
            for s in range(slots):
                accumulate(c, 1 - y, s)
            for s in range(1, slots):
                for name, h in (("across", across), ("diagonal", diagonal)):
                    arriving[name, s].wait_recv()
                    discount(h, s)
                accumulate(across, y, s)
            for s in range(slots):
                accumulate(diagonal, y, s)
    for s in range(slots):
        accumulate(across, 1 - y, s)
    for which, g in ((2, sibling), (3, diagonal)):
        for copy in given[which]:
            copy.wait_recv()
        for s in range(slots):
            accumulate(g, 1 - y, s)

    part[...] = jnp.zeros(part.shape, jnp.float32)
    for s in range(slots):
        gained = jnp.zeros((half, 128), jnp.float32)
        for tile in range(paths // 128):
            cols = slice(tile * 128, tile * 128 + 128)
            held_value = value[s, :, cols]
            square = held_value * held_value + SOFTEN
            inverse = lax.rsqrt(square)
            gained = gained + 0.5 * (held_value + square * inverse)
            steep = column[s] * (1.0 + held_value * inverse)
            slope[s, cols, :] = jnp.transpose(steep).astype(jnp.bfloat16)
        gained = jnp.sum(jnp.transpose(gained), axis=0, keepdims=True) / total_paths
        for n in range(2):
            part[2 * x + n, s : s + 1, :] = gained[:, n * 128 : n * 128 + 128]

    for s in range(slots):
        for g in range(groups):
            for m in range(0, cfg, 256):
                down = pl.ds(g * cfg + m, 256)
                pulled = jnp.dot(disc[s, down, :], slope[s], preferred_element_type=jnp.float32)
                pulled = pulled * cash[g, m : m + 256, :].astype(jnp.float32)
                summed[m : m + 256, :] = (pulled[:, :128] + pulled[:, 128:]) * pull[s, m : m + 256, :]
            whole = summed[...]
            high = whole.astype(jnp.bfloat16)
            rest = (whole - high.astype(jnp.float32)).astype(jnp.bfloat16)
            pair = jnp.dot(
                grid[s], jnp.concatenate([high, rest], axis=1), preferred_element_type=jnp.float32
            )
            spread = jnp.transpose(pair[:, :128] + pair[:, 128:])
            part[g, slots + s : slots + s + 1, :nodes] = jnp.sum(spread, axis=0, keepdims=True)

    sums = [remote(part.at[g], held.at[c, p], (g, q)) for g, q in others]
    held[c, p] = part[c]
    for copy in sums:
        copy.wait_recv()
    for d in range(dates):
        slot = date_ref[d]
        q = slot // slots
        s = slot % slots
        gains = held[2 * x, q] + held[2 * x + 1, q]
        total = held[0, q]
        for g in range(1, groups):
            total = total + held[g, q]
        gain, sens = gains[0:1], total[slots : slots + 1]
        for n in range(1, slots):
            gain = jnp.where(s == n, gains[n : n + 1], gain)
            sens = jnp.where(s == n, total[slots + n : slots + n + 1], sens)
        exp_ref[d : d + 1, :] = gain
        sens_ref[d : d + 1, :] = sens[:, :nodes]
    for copy in started:
        copy.wait_send()


def by_slot(curve_store, cash_index, cash_amount, trade_set, date_slot, default_weight):
    groups, members = lax.axis_size("ccy"), lax.axis_size("path")
    _, slots, nodes, total_paths = curve_store.shape
    trades, flows = cash_index.shape[1:]
    dates, nsets = default_weight.shape
    rows, half, paths = CFG // members, nsets // 2, total_paths // 2
    levels = members // 2
    parts = -(-2 * slots // 8) * 8
    count = 1 + 2 * (levels - 1) + 2 * levels + 4 * levels + 3 * slots + groups * members - 1
    smem = pl.BlockSpec(memory_space=pltpu.SMEM)
    vmem = pl.BlockSpec(memory_space=pltpu.VMEM)
    bf16, f32 = jnp.bfloat16, jnp.float32
    exposure, sens = pl.pallas_call(
        functools.partial(fused_kernel, total_paths),
        out_shape=[
            jax.ShapeDtypeStruct((dates, nsets // groups), f32),
            jax.ShapeDtypeStruct((dates, nodes), f32),
        ],
        in_specs=[smem] + [pl.BlockSpec(memory_space=pl.ANY)] * 5,
        out_specs=[vmem, vmem],
        scratch_shapes=[
            pltpu.VMEM((flows, trades), jnp.int32),
            pltpu.VMEM((flows, trades), f32),
            pltpu.VMEM((1, trades), jnp.int32),
            pltpu.VMEM((dates, nsets), f32),
            pltpu.VMEM((2 * rows, trades), bf16),
            pltpu.VMEM((nsets, trades), bf16),
            pltpu.VMEM((groups, CFG, half), bf16),
            pltpu.VMEM((rows, half), bf16),
            pltpu.VMEM((groups, slots, nodes, paths), bf16),
            pltpu.VMEM((slots, CFG, 4 * nodes), bf16),
            pltpu.VMEM((slots, CFG, 128), f32),
            pltpu.VMEM((slots, nodes, CFG), bf16),
            pltpu.VMEM((slots, half, 128), f32),
            pltpu.VMEM((slots, groups * CFG, paths), bf16),
            pltpu.VMEM((slots, half, paths), f32),
            pltpu.VMEM((slots, paths, half), bf16),
            pltpu.VMEM((CFG, 128), f32),
            pltpu.VMEM((groups, parts, 128), f32),
            pltpu.VMEM((groups, members, parts, 128), f32),
            pltpu.SemaphoreType.DMA((count,)),
            pltpu.SemaphoreType.DMA((count,)),
            pltpu.SemaphoreType.DMA((5,)),
        ],
        compiler_params=pltpu.CompilerParams(collective_id=0, has_side_effects=True),
        name="fused",
    )(date_slot, cash_index[0].T, cash_amount[0].T, trade_set, default_weight, curve_store[0])
    return (exposure, sens[None])


def by_path(curve_store, cash_index, cash_amount, trade_set, date_slot, default_weight):
    groups = lax.axis_size("ccy")
    group_index = lax.axis_index("ccy")
    members = lax.axis_size("path")
    nodes, total_paths = curve_store.shape[2], curve_store.shape[3]
    nsets = default_weight.shape[1]
    share_size = nsets // groups
    rows = CFG // members
    base = (lax.axis_index("path") * rows).astype(jnp.int32)[None]
    chunk = build_cash(base, cash_index[0], cash_amount[0], trade_set[0], rows, nsets)
    cash_table = lax.all_gather(chunk, "path", axis=0, tiled=True)
    blocks = lax.all_to_all(curve_store, "path", split_axis=3, concat_axis=1, tiled=True)[0]
    cash_all = lax.all_gather(cash_table[None], "ccy", axis=0, tiled=True)

    def advance(unused, inputs):
        date_index, slot_id, weight_row = inputs
        remain, alive_mask, weights = date_tables(date_index, nodes, CFG)
        grid_weights = weights.astype(jnp.bfloat16)
        curve_now = lax.dynamic_index_in_dim(blocks, slot_id, 0, keepdims=False)
        curve_groups = lax.all_gather(curve_now[None], "ccy", axis=0, tiled=True)
        yields = jnp.einsum(
            "gnp,nc->gpc", curve_groups, grid_weights, preferred_element_type=jnp.float32
        )
        discount_all = alive_mask * jnp.exp(-yields * remain)
        values = jnp.einsum(
            "gpc,gcs->ps", discount_all.astype(jnp.bfloat16), cash_all,
            preferred_element_type=jnp.float32,
        )
        discount = lax.dynamic_index_in_dim(discount_all, group_index, 0, keepdims=False)
        rooted = jnp.sqrt(values * values + SOFTEN)
        slopes = (weight_row / total_paths * 0.5 * (1.0 + values / rooted)).astype(jnp.bfloat16)
        share_values = lax.dynamic_slice_in_dim(values, group_index * share_size, share_size, 1)
        share_root = lax.dynamic_slice_in_dim(rooted, group_index * share_size, share_size, 1)
        exposure_part = jnp.sum(0.5 * (share_values + share_root), axis=0) / total_paths
        back_flow = lax.dot_general(
            slopes, cash_table, (((1,), (1,)), ((), ())), preferred_element_type=jnp.float32
        )
        node_pull = jnp.sum(back_flow * -remain * discount, axis=0)
        sens_part = jnp.dot(weights, node_pull, precision=lax.Precision.HIGHEST)
        exposure_part, sens_part = lax.psum((exposure_part, sens_part), "path")
        return (unused, (exposure_part, sens_part))

    inputs = (jnp.arange(date_slot.shape[0], dtype=jnp.int32), date_slot, default_weight)
    _, (exposure_rows, sens_rows) = lax.scan(advance, jnp.zeros((), jnp.float32), inputs)
    return (exposure_rows, sens_rows[None])


def local(curve_store, cash_index, cash_amount, trade_set, date_slot, default_weight):
    groups, members = lax.axis_size("ccy"), lax.axis_size("path")
    slots, nodes, total_paths = curve_store.shape[1:]
    nsets = default_weight.shape[1]
    trades = trade_set.shape[1]
    fits = groups == 4 and members % 2 == 0 and slots * members == date_slot.shape[0]
    fits = fits and nodes * 0.5 == HORIZON and CFG == 16 * nodes and total_paths % 256 == 0
    fits = fits and nsets == 4 * 128 and CFG // members == 128 and trades % 128 == 0
    plan = by_slot if fits else by_path
    return plan(curve_store, cash_index, cash_amount, trade_set, date_slot, default_weight)


def solution(mesh):
    in_specs = (
        P("ccy", "path", None, None),
        P("ccy", None, None),
        P("ccy", None, None),
        P("ccy", None),
        P(),
        P(),
    )
    out_specs = (P(None, "ccy"), P("ccy", None, None))
    return jax.shard_map(local, mesh=mesh, in_specs=in_specs, out_specs=out_specs, check_vma=False)
```

```python
import functools

import jax
import jax.numpy as jnp
from jax import lax
from jax.experimental import pallas as pl
from jax.experimental.pallas import tpu as pltpu
from jax.sharding import PartitionSpec as P

NSETS = 512
CFG = 1024
SOFTEN = 0.04
HORIZON = 32.0
LOG2E = 1.4426950408889634


def date_tables(date_index, node_count, grid_count):
    start_time = 0.5 * (jnp.asarray(date_index).astype(jnp.float32) + 1.0)
    grid_times = HORIZON * (jnp.arange(grid_count, dtype=jnp.float32) + 1.0) / grid_count
    tenors = HORIZON * (jnp.arange(node_count, dtype=jnp.float32) + 1.0) / node_count
    remain = grid_times - start_time
    alive_mask = (remain > 0.0).astype(jnp.float32)
    clipped = jnp.clip(remain, HORIZON / node_count, HORIZON)
    weights = jnp.maximum(
        0.0, 1.0 - jnp.abs(clipped[None, :] - tenors[:, None]) * (node_count / HORIZON)
    )
    return (remain, alive_mask, weights)


def cash_kernel(rows, base_ref, index_ref, amount_ref, set_ref, out_ref, a_hi, a_lo):
    flows, trades = index_ref.shape
    nsets = out_ref.shape[1]
    wanted = lax.broadcasted_iota(jnp.int32, (rows, 128), 0) + base_ref[0]

    @pl.loop(0, trades // 128)
    def _(tile):
        cols = pl.ds(pl.multiple_of(tile * 128, 128), 128)
        total = jnp.zeros((rows, 128), jnp.float32)
        index = index_ref[:, cols]
        amount = amount_ref[:, cols]
        for k in range(flows):
            hit = wanted == index[k : k + 1, :]
            total = total + jnp.where(hit, amount[k : k + 1, :], 0.0)
        high = total.astype(jnp.bfloat16)
        a_hi[:, cols] = high
        a_lo[:, cols] = (total - high.astype(jnp.float32)).astype(jnp.bfloat16)

    sets = lax.broadcasted_iota(jnp.int32, (nsets, trades), 0)
    onehot = jnp.where(sets == set_ref[...], 1.0, 0.0).astype(jnp.bfloat16)
    dims = (((1,), (1,)), ((), ()))
    table = lax.dot_general(a_hi[...], onehot, dims, preferred_element_type=jnp.float32)
    table = table + lax.dot_general(a_lo[...], onehot, dims, preferred_element_type=jnp.float32)
    out_ref[...] = table.astype(jnp.bfloat16)


def build_cash(base, flow_index, amount, trade_sets, rows, nsets):
    flows, trades = flow_index.shape[1], flow_index.shape[0]
    vmem = pl.BlockSpec(memory_space=pltpu.VMEM)
    return pl.pallas_call(
        functools.partial(cash_kernel, rows),
        out_shape=jax.ShapeDtypeStruct((rows, nsets), jnp.bfloat16),
        in_specs=[pl.BlockSpec(memory_space=pltpu.SMEM), vmem, vmem, vmem],
        out_specs=vmem,
        scratch_shapes=[pltpu.VMEM((rows, trades), jnp.bfloat16)] * 2,
        cost_estimate=pl.CostEstimate(
            flops=4 * rows * trades * nsets, bytes_accessed=4 * trades * flows, transcendentals=0
        ),
        name="cash_rows",
    )(base, flow_index.T, amount.T, trade_sets[None, :])


def fused_kernel(
    total_paths, date_hbm, index_hbm, amount_hbm, set_hbm, weight_hbm, curve_ref, exp_ref, sens_ref,
    date_ref, index_ref, amount_ref, set_ref, weight_ref, table, onehot, cash, other, curves, coef, pull, grid,
    column, disc, value, slope, summed, part_e, part_s, held_e, held_s, send, recv, own,
):
    groups, slots, nodes, paths = curves.shape
    flows, trades = index_ref.shape
    cfg, half = cash.shape[1], cash.shape[2]
    nsets = 2 * half
    members = held_e.shape[1]
    levels = members // 2
    rows = cfg // members
    dates = date_ref.shape[0]
    step = HORIZON / cfg
    c, p = lax.axis_index("ccy"), lax.axis_index("path")
    x, k = c // 2, c % 2
    z, y = p // 2, p % 2
    sibling = c + 1 - 2 * k
    across = (c + 2) % groups
    diagonal = (sibling + 2) % groups
    beside = p + 1 - 2 * y
    barrier = pltpu.get_barrier_semaphore()
    others = [
        ((c + dc) % groups, (p + dp) % members) for dc in range(groups) for dp in range(members)
    ][1:]
    next_level = z + 1 - 2 * (z % 2)
    far_level = (z + 2) % levels
    last_level = far_level + 1 - 2 * (far_level % 2)
    beyond, above = (c, far_level * 2 + y), (c, next_level * 2 + y)
    peers = [(sibling, p), (across, p), (diagonal, p), (c, beside), beyond, above]
    loads = [
        pltpu.make_async_copy(source, target, own.at[1 + n])
        for n, (source, target) in enumerate(
            (
                (index_hbm, index_ref), (amount_hbm, amount_ref), (set_hbm, set_ref),
                (weight_hbm, weight_ref), (date_hbm, date_ref),
            )
        )
    ]
    for load in loads:
        load.start()
    for peer in peers:
        pl.semaphore_signal(barrier, inc=1, device_id=peer, device_id_type=pl.DeviceIdType.MESH)

    started = []

    def remote(source, target, device):
        n = len(started)
        copy = pltpu.make_async_remote_copy(
            src_ref=source, dst_ref=target, send_sem=send.at[n], recv_sem=recv.at[n],
            device_id=device, device_id_type=pl.DeviceIdType.MESH,
        )
        copy.start()
        started.append(copy)
        return copy

    def lanes(which):
        return pl.ds(pl.multiple_of(which * paths, 128), paths)

    keep = pltpu.make_async_copy(curve_ref.at[:, :, lanes(k)], curves.at[c], own.at[0])
    keep.start()

    def block(g, level, side):
        at = (side * levels + level) * rows
        return cash.at[g, pl.ds(pl.multiple_of(at, 16), rows), :]

    wanted = lax.broadcasted_iota(jnp.int32, (rows, 128), 0) + (y * levels + z) * rows
    sets = lax.broadcasted_iota(jnp.int32, (nsets, 128), 0)
    for load in loads:
        load.wait()

    @pl.loop(0, trades // 128)
    def _(tile):
        cols = pl.ds(pl.multiple_of(tile * 128, 128), 128)
        total = jnp.zeros((rows, 128), jnp.float32)
        index = index_ref[:, cols]
        amount = amount_ref[:, cols]
        for n in range(flows):
            hit = wanted == index[n : n + 1, :]
            total = total + jnp.where(hit, amount[n : n + 1, :], 0.0)
        high = total.astype(jnp.bfloat16)
        table[0:rows, cols] = high
        table[rows : 2 * rows, cols] = (total - high.astype(jnp.float32)).astype(jnp.bfloat16)
        onehot[:, cols] = jnp.where(sets == set_ref[:, cols], 1.0, 0.0).astype(jnp.bfloat16)

    both = lax.dot_general(
        onehot[...], table[...], (((1,), (1,)), ((), ())), preferred_element_type=jnp.float32
    )
    netted = jnp.transpose(both[:, :rows] + both[:, rows:]).astype(jnp.bfloat16)
    here = pl.ds(pl.multiple_of((y * levels + z) * rows, 16), rows)
    low, top = netted[:, :half], netted[:, half:]
    cash[c, here, :] = jnp.where(x == 0, low, top)
    other[...] = jnp.where(x == 0, top, low)

    pl.semaphore_wait(barrier, len(peers))
    near, core, over = (c, beside), (sibling, p), (across, p)
    mine = block(c, z, y)
    crossing = remote(other, mine, over)
    sides, given = [[], []], [[], [], [], []]

    def leave(which, level, source):
        sides[which].append((level, remote(source, source, near)))
        given[which].append(remote(source, source, core))

    jump, hop, relay = [None, None], [None, None], [None, None]
    jump[0], hop[0] = remote(mine, mine, beyond), remote(mine, mine, above)
    leave(0, z, mine)
    arriving = {}
    for s in range(slots):
        arriving["sibling", s] = remote(curve_ref.at[s, :, lanes(1 - k)], curves.at[c, s], core)
    for s in range(slots):
        arriving["across", s] = remote(curve_ref.at[s, :, lanes(k)], curves.at[c, s], over)
        arriving["diagonal", s] = remote(curve_ref.at[s, :, lanes(1 - k)], curves.at[c, s], (diagonal, p))

    starts = []
    for s in range(slots):
        date = jnp.int32(0)
        for d in range(dates):
            date = date + jnp.where(date_ref[d] == p * slots + s, d, 0)
        shift = (date + 1).astype(jnp.float32)
        starts.append((date, shift))
        at = lax.broadcasted_iota(jnp.int32, (cfg, nodes), 0).astype(jnp.float32)
        after = (at + 1.0) * step - shift * (HORIZON / nodes)
        inside = jnp.clip(after, HORIZON / nodes, HORIZON)
        tenor = (lax.broadcasted_iota(jnp.int32, (cfg, nodes), 1).astype(jnp.float32) + 1.0) * (HORIZON / nodes)
        weight = jnp.maximum(0.0, 1.0 - jnp.abs(inside - tenor) * (nodes / HORIZON))
        rest = jnp.where(after > 0.0, weight * (after * -LOG2E), 0.0)
        for n in range(3):
            piece = rest.astype(jnp.bfloat16)
            rest = rest - piece.astype(jnp.float32)
            coef[s, :, n * nodes : n * nodes + nodes] = piece
        first = lax.broadcasted_iota(jnp.int32, (cfg, nodes), 1) == 0
        dead = jnp.where(first, jnp.where(after > 0.0, 0.0, -1000.0), 0.0)
        coef[s, :, 3 * nodes : 4 * nodes] = dead.astype(jnp.bfloat16)
        at = lax.broadcasted_iota(jnp.int32, (cfg, 128), 0).astype(jnp.float32)
        pull[s] = shift * (HORIZON / nodes) - (at + 1.0) * step
        flat = lax.broadcasted_iota(jnp.int32, (nodes, cfg), 1).astype(jnp.float32)
        left = jnp.clip((flat + 1.0) * step - shift * (HORIZON / nodes), HORIZON / nodes, HORIZON)
        tenors = (lax.broadcasted_iota(jnp.int32, (nodes, cfg), 0).astype(jnp.float32) + 1.0) * (HORIZON / nodes)
        grid[s] = jnp.maximum(0.0, 1.0 - jnp.abs(left - tenors) * (nodes / HORIZON)).astype(jnp.bfloat16)
        line = lax.broadcasted_iota(jnp.int32, (dates, half), 0) == date
        row = jnp.where(x == 0, weight_ref[:, :half], weight_ref[:, half:])
        row = jnp.sum(jnp.where(line, row, 0.0), axis=0, keepdims=True) / total_paths * 0.5
        column[s] = jnp.transpose(jnp.broadcast_to(row, (128, half)))

    def discount(g, s):
        curve = curves[g, s]
        lines = jnp.concatenate([curve, curve, curve, jnp.ones(curve.shape, jnp.bfloat16)], axis=0)
        for m in range(0, cfg, 256):
            power = jnp.dot(coef[s, m : m + 256, :], lines, preferred_element_type=jnp.float32)
            target = pl.ds(pl.multiple_of(g * cfg + m, 256), 256)
            disc[s, target, :] = jnp.exp2(power).astype(jnp.bfloat16)

    stretch = cfg // 2
    fresh = [True] * slots

    def accumulate(g, side, s):
        at = pl.ds(pl.multiple_of(side * stretch, 16), stretch)
        down = pl.ds(pl.multiple_of(g * cfg + side * stretch, 16), stretch)
        product = lax.dot_general(
            cash[g, at, :], disc[s, down, :], (((0,), (0,)), ((), ())), preferred_element_type=jnp.float32
        )
        if fresh[s]:
            value[s] = product
        else:
            value[s] = value[s] + product
        fresh[s] = False

    group = (c, across, sibling, diagonal)

    def relayed(which):
        jump[which].wait_recv()
        there = block(group[which], far_level, y)
        relay[which] = remote(there, there, above)
        leave(which, far_level, there)

    def reached(which, copies, level):
        copies[which].wait_recv()
        leave(which, level, block(group[which], level, y))

    def shared(which, count):
        for level, copy in sides[which][:count]:
            copy.wait_recv()
            there = block(group[which], level, 1 - y)
            given[2 + which].append(remote(there, there, core))
        del sides[which][:count]

    def landed(which):
        for copy in given[which]:
            copy.wait_recv()

    def priced(name, which, s):
        arriving[name, s].wait_recv()
        discount(group[which], s)

    keep.wait()
    for s in range(slots):
        discount(c, s)
    crossing.wait_recv()
    got = block(across, z, y)
    jump[1], hop[1] = remote(got, got, beyond), remote(got, got, above)
    leave(1, z, got)
    priced("sibling", 2, 0)
    relayed(0)
    for s in range(1, slots):
        priced("sibling", 2, s)
    reached(0, hop, next_level)
    shared(0, 1)
    priced("across", 1, 0)
    relayed(1)
    reached(0, relay, last_level)
    accumulate(c, y, 0)
    reached(1, hop, next_level)
    shared(0, 1)
    for s in range(1, slots):
        accumulate(c, y, s)
    shared(0, 1)
    landed(0)
    accumulate(sibling, y, 0)
    reached(1, relay, last_level)
    for s in range(1, slots):
        accumulate(sibling, y, s)
    shared(1, 1)
    accumulate(across, y, 0)
    priced("diagonal", 3, 0)
    shared(0, levels)
    accumulate(c, 1 - y, 0)
    shared(1, 1)
    for s in range(1, slots):
        accumulate(c, 1 - y, s)
        priced("across", 1, s)
        accumulate(across, y, s)
    shared(1, 1)
    landed(1)
    accumulate(diagonal, y, 0)
    landed(2)
    for s in range(slots):
        accumulate(sibling, 1 - y, s)
    shared(1, levels)
    for s in range(slots):
        accumulate(across, 1 - y, s)
    for s in range(1, slots):
        priced("diagonal", 3, s)
        accumulate(diagonal, y, s)
    landed(3)
    for s in range(slots):
        accumulate(diagonal, 1 - y, s)

    part_s[...] = jnp.zeros(part_s.shape, jnp.float32)
    for s in range(slots):
        gained = jnp.zeros((half, 128), jnp.float32)
        for tile in range(paths // 128):
            cols = slice(tile * 128, tile * 128 + 128)
            held_value = value[s, :, cols]
            square = held_value * held_value + SOFTEN
            inverse = lax.rsqrt(square)
            gained = gained + 0.5 * (held_value + square * inverse)
            steep = column[s] * (1.0 + held_value * inverse)
            slope[s, cols, :] = jnp.transpose(steep).astype(jnp.bfloat16)
        gained = jnp.sum(jnp.transpose(gained), axis=0, keepdims=True) / total_paths
        for n in range(2):
            part_e[n, s] = gained[:, n * 128 : n * 128 + 128]

    twins = [((k + dk) % 2, (p + dp) % members) for dk in range(2) for dp in range(members)][1:]
    sums = [remote(part_e.at[n], held_e.at[k, p], (2 * x + n, q)) for n, q in twins]
    held_e[k, p] = part_e[k]
    for s in range(slots):
        for g in range(groups):
            for m in range(0, cfg, 256):
                down = pl.ds(g * cfg + m, 256)
                pulled = jnp.dot(disc[s, down, :], slope[s], preferred_element_type=jnp.float32)
                pulled = pulled * cash[g, m : m + 256, :].astype(jnp.float32)
                summed[m : m + 256, :] = (pulled[:, :128] + pulled[:, 128:]) * pull[s, m : m + 256, :]
            whole = summed[...]
            high = whole.astype(jnp.bfloat16)
            rest = (whole - high.astype(jnp.float32)).astype(jnp.bfloat16)
            pair = jnp.dot(
                grid[s], jnp.concatenate([high, rest], axis=1), preferred_element_type=jnp.float32
            )
            spread = jnp.transpose(pair[:, :128] + pair[:, 128:])
            part_s[s, g, :, :nodes] = jnp.sum(spread, axis=0, keepdims=True)
        sums += [remote(part_s.at[s, g], held_s.at[s, c, p], (g, q)) for g, q in others]
        held_s[s, c, p] = part_s[s, c]
    for copy in sums:
        copy.wait_recv()
    for d in range(dates):
        slot = date_ref[d]
        q = slot // slots
        s = slot % slots
        exp_ref[d : d + 1, :] = held_e[0, q, s] + held_e[1, q, s]
        total = held_s[s, 0, q]
        for g in range(1, groups):
            total = total + held_s[s, g, q]
        sens_ref[d : d + 1, :] = total[:, :nodes]
    for copy in started:
        copy.wait_send()


def by_slot(curve_store, cash_index, cash_amount, trade_set, date_slot, default_weight):
    groups, members = lax.axis_size("ccy"), lax.axis_size("path")
    _, slots, nodes, total_paths = curve_store.shape
    trades, flows = cash_index.shape[1:]
    dates, nsets = default_weight.shape
    rows, half, paths = CFG // members, nsets // 2, total_paths // 2
    levels = members // 2
    count = 1 + 6 + 2 * levels + 4 * levels + 3 * slots + 2 * members - 1 + slots * (groups * members - 1)
    vmem = pl.BlockSpec(memory_space=pltpu.VMEM)
    bf16, f32 = jnp.bfloat16, jnp.float32
    operands = (date_slot, cash_index[0].T, cash_amount[0].T, trade_set, default_weight, curve_store[0])
    exposure, sens = pl.pallas_call(
        functools.partial(fused_kernel, total_paths),
        out_shape=[
            jax.ShapeDtypeStruct((dates, nsets // groups), f32),
            jax.ShapeDtypeStruct((dates, nodes), f32),
        ],
        in_specs=[pl.BlockSpec(memory_space=pltpu.HBM)] * 6,
        out_specs=[vmem, vmem],
        scratch_shapes=[
            pltpu.SMEM((dates,), jnp.int32),
            pltpu.VMEM((flows, trades), jnp.int32),
            pltpu.VMEM((flows, trades), f32),
            pltpu.VMEM((1, trades), jnp.int32),
            pltpu.VMEM((dates, nsets), f32),
            pltpu.VMEM((2 * rows, trades), bf16),
            pltpu.VMEM((nsets, trades), bf16),
            pltpu.VMEM((groups, CFG, half), bf16),
            pltpu.VMEM((rows, half), bf16),
            pltpu.VMEM((groups, slots, nodes, paths), bf16),
            pltpu.VMEM((slots, CFG, 4 * nodes), bf16),
            pltpu.VMEM((slots, CFG, 128), f32),
            pltpu.VMEM((slots, nodes, CFG), bf16),
            pltpu.VMEM((slots, half, 128), f32),
            pltpu.VMEM((slots, groups * CFG, paths), bf16),
            pltpu.VMEM((slots, half, paths), f32),
            pltpu.VMEM((slots, paths, half), bf16),
            pltpu.VMEM((CFG, 128), f32),
            pltpu.VMEM((2, slots, 1, 128), f32),
            pltpu.VMEM((slots, groups, 1, 128), f32),
            pltpu.VMEM((2, members, slots, 1, 128), f32),
            pltpu.VMEM((slots, groups, members, 1, 128), f32),
            pltpu.SemaphoreType.DMA((count,)),
            pltpu.SemaphoreType.DMA((count,)),
            pltpu.SemaphoreType.DMA((6,)),
        ],
        compiler_params=pltpu.CompilerParams(
            collective_id=0, has_side_effects=True, vmem_limit_bytes=48 * 1024 * 1024
        ),
        name="fused",
    )(*(pltpu.with_memory_space_constraint(operand, pltpu.HBM) for operand in operands))
    return (exposure, sens[None])


def by_path(curve_store, cash_index, cash_amount, trade_set, date_slot, default_weight):
    groups = lax.axis_size("ccy")
    group_index = lax.axis_index("ccy")
    members = lax.axis_size("path")
    nodes, total_paths = curve_store.shape[2], curve_store.shape[3]
    nsets = default_weight.shape[1]
    share_size = nsets // groups
    rows = CFG // members
    base = (lax.axis_index("path") * rows).astype(jnp.int32)[None]
    chunk = build_cash(base, cash_index[0], cash_amount[0], trade_set[0], rows, nsets)
    cash_table = lax.all_gather(chunk, "path", axis=0, tiled=True)
    blocks = lax.all_to_all(curve_store, "path", split_axis=3, concat_axis=1, tiled=True)[0]
    cash_all = lax.all_gather(cash_table[None], "ccy", axis=0, tiled=True)

    def advance(unused, inputs):
        date_index, slot_id, weight_row = inputs
        remain, alive_mask, weights = date_tables(date_index, nodes, CFG)
        grid_weights = weights.astype(jnp.bfloat16)
        curve_now = lax.dynamic_index_in_dim(blocks, slot_id, 0, keepdims=False)
        curve_groups = lax.all_gather(curve_now[None], "ccy", axis=0, tiled=True)
        yields = jnp.einsum(
            "gnp,nc->gpc", curve_groups, grid_weights, preferred_element_type=jnp.float32
        )
        discount_all = alive_mask * jnp.exp(-yields * remain)
        values = jnp.einsum(
            "gpc,gcs->ps", discount_all.astype(jnp.bfloat16), cash_all,
            preferred_element_type=jnp.float32,
        )
        discount = lax.dynamic_index_in_dim(discount_all, group_index, 0, keepdims=False)
        rooted = jnp.sqrt(values * values + SOFTEN)
        slopes = (weight_row / total_paths * 0.5 * (1.0 + values / rooted)).astype(jnp.bfloat16)
        share_values = lax.dynamic_slice_in_dim(values, group_index * share_size, share_size, 1)
        share_root = lax.dynamic_slice_in_dim(rooted, group_index * share_size, share_size, 1)
        exposure_part = jnp.sum(0.5 * (share_values + share_root), axis=0) / total_paths
        back_flow = lax.dot_general(
            slopes, cash_table, (((1,), (1,)), ((), ())), preferred_element_type=jnp.float32
        )
        node_pull = jnp.sum(back_flow * -remain * discount, axis=0)
        sens_part = jnp.dot(weights, node_pull, precision=lax.Precision.HIGHEST)
        exposure_part, sens_part = lax.psum((exposure_part, sens_part), "path")
        return (unused, (exposure_part, sens_part))

    inputs = (jnp.arange(date_slot.shape[0], dtype=jnp.int32), date_slot, default_weight)
    _, (exposure_rows, sens_rows) = lax.scan(advance, jnp.zeros((), jnp.float32), inputs)
    return (exposure_rows, sens_rows[None])


def local(curve_store, cash_index, cash_amount, trade_set, date_slot, default_weight):
    groups, members = lax.axis_size("ccy"), lax.axis_size("path")
    slots, nodes, total_paths = curve_store.shape[1:]
    nsets = default_weight.shape[1]
    trades = trade_set.shape[1]
    fits = groups == 4 and members == 8 and slots * members == date_slot.shape[0]
    fits = fits and nodes * 0.5 == HORIZON and CFG == 16 * nodes and total_paths % 256 == 0
    fits = fits and nsets == 4 * 128 and CFG // members == 128 and trades % 128 == 0
    plan = by_slot if fits else by_path
    return plan(curve_store, cash_index, cash_amount, trade_set, date_slot, default_weight)


def solution(mesh):
    in_specs = (
        P("ccy", "path", None, None),
        P("ccy", None, None),
        P("ccy", None, None),
        P("ccy", None),
        P(),
        P(),
    )
    out_specs = (P(None, "ccy"), P("ccy", None, None))
    return jax.shard_map(local, mesh=mesh, in_specs=in_specs, out_specs=out_specs, check_vma=False)
```

```python
import functools

import jax
import jax.numpy as jnp
from jax import lax
from jax.experimental import pallas as pl
from jax.experimental.pallas import tpu as pltpu
from jax.sharding import PartitionSpec as P

NSETS = 512
CFG = 1024
SOFTEN = 0.04
HORIZON = 32.0
LOG2E = 1.4426950408889634


def date_tables(date_index, node_count, grid_count):
    start_time = 0.5 * (jnp.asarray(date_index).astype(jnp.float32) + 1.0)
    grid_times = HORIZON * (jnp.arange(grid_count, dtype=jnp.float32) + 1.0) / grid_count
    tenors = HORIZON * (jnp.arange(node_count, dtype=jnp.float32) + 1.0) / node_count
    remain = grid_times - start_time
    alive_mask = (remain > 0.0).astype(jnp.float32)
    clipped = jnp.clip(remain, HORIZON / node_count, HORIZON)
    weights = jnp.maximum(
        0.0, 1.0 - jnp.abs(clipped[None, :] - tenors[:, None]) * (node_count / HORIZON)
    )
    return (remain, alive_mask, weights)


def cash_kernel(rows, base_ref, index_ref, amount_ref, set_ref, out_ref, a_hi, a_lo):
    flows, trades = index_ref.shape
    nsets = out_ref.shape[1]
    wanted = lax.broadcasted_iota(jnp.int32, (rows, 128), 0) + base_ref[0]

    @pl.loop(0, trades // 128)
    def _(tile):
        cols = pl.ds(pl.multiple_of(tile * 128, 128), 128)
        total = jnp.zeros((rows, 128), jnp.float32)
        index = index_ref[:, cols]
        amount = amount_ref[:, cols]
        for k in range(flows):
            hit = wanted == index[k : k + 1, :]
            total = total + jnp.where(hit, amount[k : k + 1, :], 0.0)
        high = total.astype(jnp.bfloat16)
        a_hi[:, cols] = high
        a_lo[:, cols] = (total - high.astype(jnp.float32)).astype(jnp.bfloat16)

    sets = lax.broadcasted_iota(jnp.int32, (nsets, trades), 0)
    onehot = jnp.where(sets == set_ref[...], 1.0, 0.0).astype(jnp.bfloat16)
    dims = (((1,), (1,)), ((), ()))
    table = lax.dot_general(a_hi[...], onehot, dims, preferred_element_type=jnp.float32)
    table = table + lax.dot_general(a_lo[...], onehot, dims, preferred_element_type=jnp.float32)
    out_ref[...] = table.astype(jnp.bfloat16)


def build_cash(base, flow_index, amount, trade_sets, rows, nsets):
    flows, trades = flow_index.shape[1], flow_index.shape[0]
    vmem = pl.BlockSpec(memory_space=pltpu.VMEM)
    return pl.pallas_call(
        functools.partial(cash_kernel, rows),
        out_shape=jax.ShapeDtypeStruct((rows, nsets), jnp.bfloat16),
        in_specs=[pl.BlockSpec(memory_space=pltpu.SMEM), vmem, vmem, vmem],
        out_specs=vmem,
        scratch_shapes=[pltpu.VMEM((rows, trades), jnp.bfloat16)] * 2,
        cost_estimate=pl.CostEstimate(
            flops=4 * rows * trades * nsets, bytes_accessed=4 * trades * flows, transcendentals=0
        ),
        name="cash_rows",
    )(base, flow_index.T, amount.T, trade_sets[None, :])


def fused_kernel(
    total_paths, date_hbm, index_hbm, amount_hbm, set_hbm, weight_hbm, curve_ref, exp_ref, sens_ref,
    date_ref, index_ref, amount_ref, set_ref, weight_ref, table, onehot, cash, other, curves, coef, pull, grid,
    column, disc, value, slope, summed, part_e, part_s, held_e, held_s, send, recv, own,
):
    groups, slots, nodes, paths = curves.shape
    flows, trades = index_ref.shape
    cfg, half = cash.shape[1], cash.shape[2]
    nsets = 2 * half
    members = held_e.shape[1]
    levels = members // 2
    rows = cfg // members
    dates = date_ref.shape[0]
    step = HORIZON / cfg
    c, p = lax.axis_index("ccy"), lax.axis_index("path")
    x, k = c // 2, c % 2
    z, y = p // 2, p % 2
    sibling = c + 1 - 2 * k
    across = (c + 2) % groups
    diagonal = (sibling + 2) % groups
    beside = p + 1 - 2 * y
    barrier = pltpu.get_barrier_semaphore()
    others = [
        ((c + dc) % groups, (p + dp) % members) for dc in range(groups) for dp in range(members)
    ][1:]
    next_level = z + 1 - 2 * (z % 2)
    far_level = (z + 2) % levels
    last_level = far_level + 1 - 2 * (far_level % 2)
    beyond, above = (c, far_level * 2 + y), (c, next_level * 2 + y)
    peers = [(sibling, p), (across, p), (diagonal, p), (c, beside), beyond, above]
    loads = [
        pltpu.make_async_copy(source, target, own.at[1 + n])
        for n, (source, target) in enumerate(
            (
                (index_hbm, index_ref), (amount_hbm, amount_ref), (set_hbm, set_ref),
                (weight_hbm, weight_ref), (date_hbm, date_ref),
            )
        )
    ]
    for load in loads:
        load.start()
    for peer in peers:
        pl.semaphore_signal(barrier, inc=1, device_id=peer, device_id_type=pl.DeviceIdType.MESH)

    started = []

    def remote(source, target, device):
        n = len(started)
        copy = pltpu.make_async_remote_copy(
            src_ref=source, dst_ref=target, send_sem=send.at[n], recv_sem=recv.at[n],
            device_id=device, device_id_type=pl.DeviceIdType.MESH,
        )
        copy.start()
        started.append(copy)
        return copy

    def lanes(which):
        return pl.ds(pl.multiple_of(which * paths, 128), paths)

    keep = pltpu.make_async_copy(curve_ref.at[:, :, lanes(k)], curves.at[c], own.at[0])
    keep.start()

    def block(g, level, side):
        at = (side * levels + level) * rows
        return cash.at[g, pl.ds(pl.multiple_of(at, 16), rows), :]

    wanted = lax.broadcasted_iota(jnp.int32, (rows, 128), 0) + (y * levels + z) * rows
    sets = lax.broadcasted_iota(jnp.int32, (nsets, 128), 0)
    for load in loads:
        load.wait()

    def net(tile):
        cols = pl.ds(pl.multiple_of(tile * 128, 128), 128)
        total = jnp.zeros((rows, 128), jnp.float32)
        index = index_ref[:, cols]
        amount = amount_ref[:, cols]
        for n in range(flows):
            hit = wanted == index[n : n + 1, :]
            total = total + jnp.where(hit, amount[n : n + 1, :], 0.0)
        high = total.astype(jnp.bfloat16)
        table[0:rows, cols] = high
        table[rows : 2 * rows, cols] = (total - high.astype(jnp.float32)).astype(jnp.bfloat16)
        onehot[:, cols] = jnp.where(sets == set_ref[:, cols], 1.0, 0.0).astype(jnp.bfloat16)

    near, core, over = (c, beside), (sibling, p), (across, p)
    tiles = trades // 128
    pl.loop(0, tiles // 2)(net)
    pl.semaphore_wait(barrier, len(peers))
    arriving = {}
    for s in range(slots):
        arriving["sibling", s] = [remote(curve_ref.at[s, :, lanes(1 - k)], curves.at[c, s], core)]

    def sent(s, start, stop):
        source = pl.ds(pl.multiple_of(k * paths + start, 128), stop - start)
        return remote(curve_ref.at[s, :, source], curves.at[c, s, :, start:stop], over)

    split = paths // 256 * 128
    arriving["across", 0] = [sent(0, 0, split)]
    pl.loop(tiles // 2, tiles)(net)
    both = lax.dot_general(
        onehot[...], table[...], (((1,), (1,)), ((), ())), preferred_element_type=jnp.float32
    )
    netted = jnp.transpose(both[:, :rows] + both[:, rows:]).astype(jnp.bfloat16)
    here = pl.ds(pl.multiple_of((y * levels + z) * rows, 16), rows)
    low, top = netted[:, :half], netted[:, half:]
    cash[c, here, :] = jnp.where(x == 0, low, top)
    other[...] = jnp.where(x == 0, top, low)

    mine = block(c, z, y)
    crossing = remote(other, mine, over)
    sides, given = [[], []], [[], [], [], []]

    def leave(which, level, source):
        sides[which].append((level, remote(source, source, near)))
        given[which].append(remote(source, source, core))

    jump, hop, relay = [None, None], [None, None], [None, None]
    jump[0], hop[0] = remote(mine, mine, beyond), remote(mine, mine, above)
    leave(0, z, mine)
    for s in range(slots):
        arriving.setdefault(("across", s), []).append(sent(s, split if s == 0 else 0, paths))
        arriving["diagonal", s] = [remote(curve_ref.at[s, :, lanes(1 - k)], curves.at[c, s], (diagonal, p))]

    starts = []
    for s in range(slots):
        date = jnp.int32(0)
        for d in range(dates):
            date = date + jnp.where(date_ref[d] == p * slots + s, d, 0)
        shift = (date + 1).astype(jnp.float32)
        starts.append((date, shift))
        at = lax.broadcasted_iota(jnp.int32, (cfg, nodes), 0).astype(jnp.float32)
        after = (at + 1.0) * step - shift * (HORIZON / nodes)
        inside = jnp.clip(after, HORIZON / nodes, HORIZON)
        tenor = (lax.broadcasted_iota(jnp.int32, (cfg, nodes), 1).astype(jnp.float32) + 1.0) * (HORIZON / nodes)
        weight = jnp.maximum(0.0, 1.0 - jnp.abs(inside - tenor) * (nodes / HORIZON))
        rest = jnp.where(after > 0.0, weight * (after * -LOG2E), 0.0)
        for n in range(3):
            piece = rest.astype(jnp.bfloat16)
            rest = rest - piece.astype(jnp.float32)
            coef[s, :, n * nodes : n * nodes + nodes] = piece
        first = lax.broadcasted_iota(jnp.int32, (cfg, nodes), 1) == 0
        dead = jnp.where(first, jnp.where(after > 0.0, 0.0, -1000.0), 0.0)
        coef[s, :, 3 * nodes : 4 * nodes] = dead.astype(jnp.bfloat16)
        at = lax.broadcasted_iota(jnp.int32, (cfg, 128), 0).astype(jnp.float32)
        pull[s] = shift * (HORIZON / nodes) - (at + 1.0) * step
        flat = lax.broadcasted_iota(jnp.int32, (nodes, cfg), 1).astype(jnp.float32)
        left = jnp.clip((flat + 1.0) * step - shift * (HORIZON / nodes), HORIZON / nodes, HORIZON)
        tenors = (lax.broadcasted_iota(jnp.int32, (nodes, cfg), 0).astype(jnp.float32) + 1.0) * (HORIZON / nodes)
        grid[s] = jnp.maximum(0.0, 1.0 - jnp.abs(left - tenors) * (nodes / HORIZON)).astype(jnp.bfloat16)
        line = lax.broadcasted_iota(jnp.int32, (dates, half), 0) == date
        row = jnp.where(x == 0, weight_ref[:, :half], weight_ref[:, half:])
        row = jnp.sum(jnp.where(line, row, 0.0), axis=0, keepdims=True) / total_paths * 0.5
        column[s] = jnp.transpose(jnp.broadcast_to(row, (128, half)))

    def discount(g, s):
        curve = curves[g, s]
        lines = jnp.concatenate([curve, curve, curve, jnp.ones(curve.shape, jnp.bfloat16)], axis=0)
        for m in range(0, cfg, 256):
            power = jnp.dot(coef[s, m : m + 256, :], lines, preferred_element_type=jnp.float32)
            target = pl.ds(pl.multiple_of(g * cfg + m, 256), 256)
            disc[s, target, :] = jnp.exp2(power).astype(jnp.bfloat16)

    stretch = cfg // 2
    fresh = [True] * slots

    def accumulate(g, side, s, level=None):
        extent = stretch if level is None else 2 * rows
        base = side * stretch + (0 if level is None else level // 2 * extent)
        at = pl.ds(pl.multiple_of(base, 16), extent)
        down = pl.ds(pl.multiple_of(g * cfg + base, 16), extent)
        product = lax.dot_general(
            cash[g, at, :], disc[s, down, :], (((0,), (0,)), ((), ())), preferred_element_type=jnp.float32
        )
        if fresh[s]:
            value[s] = product
        else:
            value[s] = value[s] + product
        fresh[s] = False

    group = (c, across, sibling, diagonal)

    def relayed(which):
        jump[which].wait_recv()
        there = block(group[which], far_level, y)
        relay[which] = remote(there, there, above)
        leave(which, far_level, there)

    def reached(which, copies, level):
        copies[which].wait_recv()
        leave(which, level, block(group[which], level, y))

    def shared(which, count):
        for level, copy in sides[which][:count]:
            copy.wait_recv()
            there = block(group[which], level, 1 - y)
            given[2 + which].append(remote(there, there, core))
        del sides[which][:count]

    def landed(which, count=None):
        for copy in given[which][:count]:
            copy.wait_recv()
        del given[which][:count]

    def priced(name, which, s):
        for copy in arriving[name, s]:
            copy.wait_recv()
        discount(group[which], s)

    keep.wait()
    for s in range(slots):
        discount(c, s)
    crossing.wait_recv()
    got = block(across, z, y)
    jump[1], hop[1] = remote(got, got, beyond), remote(got, got, above)
    leave(1, z, got)
    priced("sibling", 2, 0)
    relayed(0)
    for s in range(1, slots):
        priced("sibling", 2, s)
    reached(0, hop, next_level)
    shared(0, 1)
    priced("across", 1, 0)
    relayed(1)
    reached(0, relay, last_level)
    accumulate(c, y, 0)
    reached(1, hop, next_level)
    shared(0, 1)
    for s in range(1, slots):
        accumulate(c, y, s)
    shared(0, 1)
    landed(0)
    accumulate(sibling, y, 0)
    reached(1, relay, last_level)
    for s in range(1, slots):
        accumulate(sibling, y, s)
    shared(1, 1)
    accumulate(across, y, 0)
    priced("diagonal", 3, 0)
    shared(0, levels)
    accumulate(c, 1 - y, 0)
    shared(1, 1)
    for s in range(1, slots):
        accumulate(c, 1 - y, s)
        priced("across", 1, s)
        accumulate(across, y, s)
    shared(1, 1)
    landed(1)
    accumulate(diagonal, y, 0)
    landed(2)
    for s in range(slots):
        accumulate(sibling, 1 - y, s)
    shared(1, 1)
    for s in range(slots):
        accumulate(across, 1 - y, s, z)
    for s in range(1, slots):
        priced("diagonal", 3, s)
        accumulate(diagonal, y, s)
    shared(1, levels)
    landed(3, 3)
    for s in range(slots):
        accumulate(diagonal, 1 - y, s, z)
    for s in range(slots):
        accumulate(across, 1 - y, s, far_level)
    landed(3)
    for s in range(slots):
        accumulate(diagonal, 1 - y, s, far_level)

    part_s[...] = jnp.zeros(part_s.shape, jnp.float32)
    for s in range(slots):
        gained = jnp.zeros((half, 128), jnp.float32)
        for tile in range(paths // 128):
            cols = slice(tile * 128, tile * 128 + 128)
            held_value = value[s, :, cols]
            square = held_value * held_value + SOFTEN
            inverse = lax.rsqrt(square)
            gained = gained + 0.5 * (held_value + square * inverse)
            steep = column[s] * (1.0 + held_value * inverse)
            slope[s, cols, :] = jnp.transpose(steep).astype(jnp.bfloat16)
        gained = jnp.sum(jnp.transpose(gained), axis=0, keepdims=True) / total_paths
        for n in range(2):
            part_e[n, s] = gained[:, n * 128 : n * 128 + 128]

    twins = [((k + dk) % 2, (p + dp) % members) for dk in range(2) for dp in range(members)][1:]
    sums = [remote(part_e.at[n], held_e.at[k, p], (2 * x + n, q)) for n, q in twins]
    held_e[k, p] = part_e[k]
    for s in range(slots):
        for g in range(groups):
            for m in range(0, cfg, 256):
                down = pl.ds(g * cfg + m, 256)
                pulled = jnp.dot(disc[s, down, :], slope[s], preferred_element_type=jnp.float32)
                pulled = pulled * cash[g, m : m + 256, :].astype(jnp.float32)
                summed[g, m : m + 256, :] = (pulled[:, :128] + pulled[:, 128:]) * pull[s, m : m + 256, :]
            whole = summed[g]
            high = whole.astype(jnp.bfloat16)
            rest = (whole - high.astype(jnp.float32)).astype(jnp.bfloat16)
            pair = jnp.dot(
                grid[s], jnp.concatenate([high, rest], axis=1), preferred_element_type=jnp.float32
            )
            spread = jnp.transpose(pair[:, :128] + pair[:, 128:])
            part_s[s, g, :, :nodes] = jnp.sum(spread, axis=0, keepdims=True)
        sums += [remote(part_s.at[s, g], held_s.at[s, c, p], (g, q)) for g, q in others]
        held_s[s, c, p] = part_s[s, c]
    for copy in sums:
        copy.wait_recv()
    for d in range(dates):
        slot = date_ref[d]
        q = slot // slots
        s = slot % slots
        exp_ref[d : d + 1, :] = held_e[0, q, s] + held_e[1, q, s]
        total = held_s[s, 0, q]
        for g in range(1, groups):
            total = total + held_s[s, g, q]
        sens_ref[d : d + 1, :] = total[:, :nodes]
    for copy in started:
        copy.wait_send()


def settle_kernel(exposure_ref, sens_ref, exposure_out, sens_out, done):
    copies = [
        pltpu.make_async_copy(exposure_ref, exposure_out, done.at[0]),
        pltpu.make_async_copy(sens_ref, sens_out, done.at[1]),
    ]
    for copy in copies:
        copy.start()
    for copy in copies:
        copy.wait()


def by_slot(curve_store, cash_index, cash_amount, trade_set, date_slot, default_weight):
    groups, members = lax.axis_size("ccy"), lax.axis_size("path")
    _, slots, nodes, total_paths = curve_store.shape
    trades, flows = cash_index.shape[1:]
    dates, nsets = default_weight.shape
    rows, half, paths = CFG // members, nsets // 2, total_paths // 2
    levels = members // 2
    count = 1 + 7 + 2 * levels + 4 * levels + 3 * slots + 2 * members - 1 + slots * (groups * members - 1)
    vmem = pl.BlockSpec(memory_space=pltpu.VMEM)
    bf16, f32 = jnp.bfloat16, jnp.float32
    operands = (date_slot, cash_index[0].T, cash_amount[0].T, trade_set, default_weight, curve_store[0])
    exposure, sens = pl.pallas_call(
        functools.partial(fused_kernel, total_paths),
        out_shape=[
            jax.ShapeDtypeStruct((dates, nsets // groups), f32),
            jax.ShapeDtypeStruct((dates, nodes), f32),
        ],
        in_specs=[pl.BlockSpec(memory_space=pltpu.HBM)] * 6,
        out_specs=[vmem, vmem],
        scratch_shapes=[
            pltpu.SMEM((dates,), jnp.int32),
            pltpu.VMEM((flows, trades), jnp.int32),
            pltpu.VMEM((flows, trades), f32),
            pltpu.VMEM((1, trades), jnp.int32),
            pltpu.VMEM((dates, nsets), f32),
            pltpu.VMEM((2 * rows, trades), bf16),
            pltpu.VMEM((nsets, trades), bf16),
            pltpu.VMEM((groups, CFG, half), bf16),
            pltpu.VMEM((rows, half), bf16),
            pltpu.VMEM((groups, slots, nodes, paths), bf16),
            pltpu.VMEM((slots, CFG, 4 * nodes), bf16),
            pltpu.VMEM((slots, CFG, 128), f32),
            pltpu.VMEM((slots, nodes, CFG), bf16),
            pltpu.VMEM((slots, half, 128), f32),
            pltpu.VMEM((slots, groups * CFG, paths), bf16),
            pltpu.VMEM((slots, half, paths), f32),
            pltpu.VMEM((slots, paths, half), bf16),
            pltpu.VMEM((groups, CFG, 128), f32),
            pltpu.VMEM((2, slots, 1, 128), f32),
            pltpu.VMEM((slots, groups, 1, 128), f32),
            pltpu.VMEM((2, members, slots, 1, 128), f32),
            pltpu.VMEM((slots, groups, members, 1, 128), f32),
            pltpu.SemaphoreType.DMA((count,)),
            pltpu.SemaphoreType.DMA((count,)),
            pltpu.SemaphoreType.DMA((6,)),
        ],
        compiler_params=pltpu.CompilerParams(
            collective_id=0, has_side_effects=True, vmem_limit_bytes=48 * 1024 * 1024
        ),
        name="fused",
    )(*(pltpu.with_memory_space_constraint(operand, pltpu.HBM) for operand in operands))
    exposure, sens = pl.pallas_call(
        settle_kernel,
        out_shape=[jax.ShapeDtypeStruct(array.shape, array.dtype) for array in (exposure, sens)],
        in_specs=[vmem, vmem],
        out_specs=[pl.BlockSpec(memory_space=pltpu.HBM)] * 2,
        scratch_shapes=[pltpu.SemaphoreType.DMA((2,))],
        compiler_params=pltpu.CompilerParams(vmem_limit_bytes=1024 * 1024),
        name="settle",
    )(exposure, sens)
    return (exposure, sens[None])


def by_path(curve_store, cash_index, cash_amount, trade_set, date_slot, default_weight):
    groups = lax.axis_size("ccy")
    group_index = lax.axis_index("ccy")
    members = lax.axis_size("path")
    nodes, total_paths = curve_store.shape[2], curve_store.shape[3]
    nsets = default_weight.shape[1]
    share_size = nsets // groups
    rows = CFG // members
    base = (lax.axis_index("path") * rows).astype(jnp.int32)[None]
    chunk = build_cash(base, cash_index[0], cash_amount[0], trade_set[0], rows, nsets)
    cash_table = lax.all_gather(chunk, "path", axis=0, tiled=True)
    blocks = lax.all_to_all(curve_store, "path", split_axis=3, concat_axis=1, tiled=True)[0]
    cash_all = lax.all_gather(cash_table[None], "ccy", axis=0, tiled=True)

    def advance(unused, inputs):
        date_index, slot_id, weight_row = inputs
        remain, alive_mask, weights = date_tables(date_index, nodes, CFG)
        grid_weights = weights.astype(jnp.bfloat16)
        curve_now = lax.dynamic_index_in_dim(blocks, slot_id, 0, keepdims=False)
        curve_groups = lax.all_gather(curve_now[None], "ccy", axis=0, tiled=True)
        yields = jnp.einsum(
            "gnp,nc->gpc", curve_groups, grid_weights, preferred_element_type=jnp.float32
        )
        discount_all = alive_mask * jnp.exp(-yields * remain)
        values = jnp.einsum(
            "gpc,gcs->ps", discount_all.astype(jnp.bfloat16), cash_all,
            preferred_element_type=jnp.float32,
        )
        discount = lax.dynamic_index_in_dim(discount_all, group_index, 0, keepdims=False)
        rooted = jnp.sqrt(values * values + SOFTEN)
        slopes = (weight_row / total_paths * 0.5 * (1.0 + values / rooted)).astype(jnp.bfloat16)
        share_values = lax.dynamic_slice_in_dim(values, group_index * share_size, share_size, 1)
        share_root = lax.dynamic_slice_in_dim(rooted, group_index * share_size, share_size, 1)
        exposure_part = jnp.sum(0.5 * (share_values + share_root), axis=0) / total_paths
        back_flow = lax.dot_general(
            slopes, cash_table, (((1,), (1,)), ((), ())), preferred_element_type=jnp.float32
        )
        node_pull = jnp.sum(back_flow * -remain * discount, axis=0)
        sens_part = jnp.dot(weights, node_pull, precision=lax.Precision.HIGHEST)
        exposure_part, sens_part = lax.psum((exposure_part, sens_part), "path")
        return (unused, (exposure_part, sens_part))

    inputs = (jnp.arange(date_slot.shape[0], dtype=jnp.int32), date_slot, default_weight)
    _, (exposure_rows, sens_rows) = lax.scan(advance, jnp.zeros((), jnp.float32), inputs)
    return (exposure_rows, sens_rows[None])


def local(curve_store, cash_index, cash_amount, trade_set, date_slot, default_weight):
    groups, members = lax.axis_size("ccy"), lax.axis_size("path")
    slots, nodes, total_paths = curve_store.shape[1:]
    nsets = default_weight.shape[1]
    trades = trade_set.shape[1]
    fits = groups == 4 and members == 8 and slots * members == date_slot.shape[0]
    fits = fits and nodes * 0.5 == HORIZON and CFG == 16 * nodes and total_paths % 256 == 0
    fits = fits and nsets == 4 * 128 and CFG // members == 128 and trades % 128 == 0
    plan = by_slot if fits else by_path
    return plan(curve_store, cash_index, cash_amount, trade_set, date_slot, default_weight)


def solution(mesh):
    in_specs = (
        P("ccy", "path", None, None),
        P("ccy", None, None),
        P("ccy", None, None),
        P("ccy", None),
        P(),
        P(),
    )
    out_specs = (P(None, "ccy"), P("ccy", None, None))
    return jax.shard_map(local, mesh=mesh, in_specs=in_specs, out_specs=out_specs, check_vma=False)
```

```python
import functools

import jax
import jax.numpy as jnp
from jax import lax
from jax.experimental import pallas as pl
from jax.experimental.pallas import tpu as pltpu
from jax.sharding import PartitionSpec as P

NSETS = 512
CFG = 1024
SOFTEN = 0.04
HORIZON = 32.0
LOG2E = 1.4426950408889634


def date_tables(date_index, node_count, grid_count):
    start_time = 0.5 * (jnp.asarray(date_index).astype(jnp.float32) + 1.0)
    grid_times = HORIZON * (jnp.arange(grid_count, dtype=jnp.float32) + 1.0) / grid_count
    tenors = HORIZON * (jnp.arange(node_count, dtype=jnp.float32) + 1.0) / node_count
    remain = grid_times - start_time
    alive_mask = (remain > 0.0).astype(jnp.float32)
    clipped = jnp.clip(remain, HORIZON / node_count, HORIZON)
    weights = jnp.maximum(
        0.0, 1.0 - jnp.abs(clipped[None, :] - tenors[:, None]) * (node_count / HORIZON)
    )
    return (remain, alive_mask, weights)


def cash_kernel(rows, base_ref, index_ref, amount_ref, set_ref, out_ref, a_hi, a_lo):
    flows, trades = index_ref.shape
    nsets = out_ref.shape[1]
    wanted = lax.broadcasted_iota(jnp.int32, (rows, 128), 0) + base_ref[0]

    @pl.loop(0, trades // 128)
    def _(tile):
        cols = pl.ds(pl.multiple_of(tile * 128, 128), 128)
        total = jnp.zeros((rows, 128), jnp.float32)
        index = index_ref[:, cols]
        amount = amount_ref[:, cols]
        for k in range(flows):
            hit = wanted == index[k : k + 1, :]
            total = total + jnp.where(hit, amount[k : k + 1, :], 0.0)
        high = total.astype(jnp.bfloat16)
        a_hi[:, cols] = high
        a_lo[:, cols] = (total - high.astype(jnp.float32)).astype(jnp.bfloat16)

    sets = lax.broadcasted_iota(jnp.int32, (nsets, trades), 0)
    onehot = jnp.where(sets == set_ref[...], 1.0, 0.0).astype(jnp.bfloat16)
    dims = (((1,), (1,)), ((), ()))
    table = lax.dot_general(a_hi[...], onehot, dims, preferred_element_type=jnp.float32)
    table = table + lax.dot_general(a_lo[...], onehot, dims, preferred_element_type=jnp.float32)
    out_ref[...] = table.astype(jnp.bfloat16)


def build_cash(base, flow_index, amount, trade_sets, rows, nsets):
    flows, trades = flow_index.shape[1], flow_index.shape[0]
    vmem = pl.BlockSpec(memory_space=pltpu.VMEM)
    return pl.pallas_call(
        functools.partial(cash_kernel, rows),
        out_shape=jax.ShapeDtypeStruct((rows, nsets), jnp.bfloat16),
        in_specs=[pl.BlockSpec(memory_space=pltpu.SMEM), vmem, vmem, vmem],
        out_specs=vmem,
        scratch_shapes=[pltpu.VMEM((rows, trades), jnp.bfloat16)] * 2,
        cost_estimate=pl.CostEstimate(
            flops=4 * rows * trades * nsets, bytes_accessed=4 * trades * flows, transcendentals=0
        ),
        name="cash_rows",
    )(base, flow_index.T, amount.T, trade_sets[None, :])


def fused_kernel(
    total_paths, date_hbm, index_hbm, amount_hbm, set_hbm, weight_hbm, curve_ref, exp_ref, sens_ref,
    date_ref, index_ref, amount_ref, set_ref, weight_ref, table, onehot, cash, other, curves, coef, pull, grid,
    column, disc, value, slope, summed, part_e, part_s, held_e, held_s, send, recv, own,
):
    groups, slots, nodes, paths = curves.shape
    flows, trades = index_ref.shape
    cfg, half = cash.shape[1], cash.shape[2]
    nsets = 2 * half
    members = held_e.shape[1]
    levels = members // 2
    rows = cfg // members
    dates = date_ref.shape[0]
    step = HORIZON / cfg
    c, p = lax.axis_index("ccy"), lax.axis_index("path")
    x, k = c // 2, c % 2
    z, y = p // 2, p % 2
    sibling = c + 1 - 2 * k
    across = (c + 2) % groups
    diagonal = (sibling + 2) % groups
    beside = p + 1 - 2 * y
    barrier = pltpu.get_barrier_semaphore()
    others = [
        ((c + dc) % groups, (p + dp) % members) for dc in range(groups) for dp in range(members)
    ][1:]
    next_level = z + 1 - 2 * (z % 2)
    far_level = (z + 2) % levels
    last_level = far_level + 1 - 2 * (far_level % 2)
    beyond, above = (c, far_level * 2 + y), (c, next_level * 2 + y)
    peers = [(sibling, p), (across, p), (diagonal, p), (c, beside), beyond, above]
    loads = [
        pltpu.make_async_copy(source, target, own.at[1 + n])
        for n, (source, target) in enumerate(
            (
                (index_hbm, index_ref), (amount_hbm, amount_ref), (set_hbm, set_ref),
                (weight_hbm, weight_ref), (date_hbm, date_ref),
            )
        )
    ]
    for load in loads:
        load.start()
    for peer in peers:
        pl.semaphore_signal(barrier, inc=1, device_id=peer, device_id_type=pl.DeviceIdType.MESH)

    started = []

    def remote(source, target, device):
        n = len(started)
        copy = pltpu.make_async_remote_copy(
            src_ref=source, dst_ref=target, send_sem=send.at[n], recv_sem=recv.at[n],
            device_id=device, device_id_type=pl.DeviceIdType.MESH,
        )
        copy.start()
        started.append(copy)
        return copy

    def lanes(which):
        return pl.ds(pl.multiple_of(which * paths, 128), paths)

    keep = pltpu.make_async_copy(curve_ref.at[:, :, lanes(k)], curves.at[c], own.at[0])
    keep.start()

    def block(g, level, side):
        at = (side * levels + level) * rows
        return cash.at[g, pl.ds(pl.multiple_of(at, 16), rows), :]

    wanted = lax.broadcasted_iota(jnp.int32, (rows, 128), 0) + (y * levels + z) * rows
    sets = lax.broadcasted_iota(jnp.int32, (nsets, 128), 0)
    for load in loads:
        load.wait()

    def net(tile):
        cols = pl.ds(pl.multiple_of(tile * 128, 128), 128)
        total = jnp.zeros((rows, 128), jnp.float32)
        index = index_ref[:, cols]
        amount = amount_ref[:, cols]
        for n in range(flows):
            hit = wanted == index[n : n + 1, :]
            total = total + jnp.where(hit, amount[n : n + 1, :], 0.0)
        high = total.astype(jnp.bfloat16)
        table[0:rows, cols] = high
        table[rows : 2 * rows, cols] = (total - high.astype(jnp.float32)).astype(jnp.bfloat16)
        onehot[:, cols] = jnp.where(sets == set_ref[:, cols], 1.0, 0.0).astype(jnp.bfloat16)

    near, core, over = (c, beside), (sibling, p), (across, p)
    tiles = trades // 128
    pl.loop(0, tiles)(net)
    both = lax.dot_general(
        onehot[...], table[...], (((1,), (1,)), ((), ())), preferred_element_type=jnp.float32
    )
    netted = jnp.transpose(both[:, :rows] + both[:, rows:]).astype(jnp.bfloat16)
    here = pl.ds(pl.multiple_of((y * levels + z) * rows, 16), rows)
    low, top = netted[:, :half], netted[:, half:]
    cash[c, here, :] = jnp.where(x == 0, low, top)
    other[...] = jnp.where(x == 0, top, low)

    pl.semaphore_wait(barrier, len(peers))
    mine = block(c, z, y)
    crossing = remote(other, mine, over)
    sides, given = [[], []], [[], [], [], []]

    def leave(which, level, source):
        sides[which].append((level, remote(source, source, near)))
        given[which].append(remote(source, source, core))

    jump, hop, relay = [None, None], [None, None], [None, None]
    jump[0], hop[0] = remote(mine, mine, beyond), remote(mine, mine, above)
    leave(0, z, mine)
    arriving = {}
    for s in range(slots):
        arriving["sibling", s] = [remote(curve_ref.at[s, :, lanes(1 - k)], curves.at[c, s], core)]

    def sent(s, start, stop):
        source = pl.ds(pl.multiple_of(k * paths + start, 128), stop - start)
        return remote(curve_ref.at[s, :, source], curves.at[c, s, :, start:stop], over)

    for s in range(slots):
        arriving.setdefault(("across", s), []).append(sent(s, 0, paths))
        arriving["diagonal", s] = [remote(curve_ref.at[s, :, lanes(1 - k)], curves.at[c, s], (diagonal, p))]

    starts = []
    for s in range(slots):
        date = jnp.int32(0)
        for d in range(dates):
            date = date + jnp.where(date_ref[d] == p * slots + s, d, 0)
        shift = (date + 1).astype(jnp.float32)
        starts.append((date, shift))
        at = lax.broadcasted_iota(jnp.int32, (cfg, nodes), 0).astype(jnp.float32)
        after = (at + 1.0) * step - shift * (HORIZON / nodes)
        inside = jnp.clip(after, HORIZON / nodes, HORIZON)
        tenor = (lax.broadcasted_iota(jnp.int32, (cfg, nodes), 1).astype(jnp.float32) + 1.0) * (HORIZON / nodes)
        weight = jnp.maximum(0.0, 1.0 - jnp.abs(inside - tenor) * (nodes / HORIZON))
        rest = jnp.where(after > 0.0, weight * (after * -LOG2E), 0.0)
        for n in range(3):
            piece = rest.astype(jnp.bfloat16)
            rest = rest - piece.astype(jnp.float32)
            coef[s, :, n * nodes : n * nodes + nodes] = piece
        first = lax.broadcasted_iota(jnp.int32, (cfg, nodes), 1) == 0
        dead = jnp.where(first, jnp.where(after > 0.0, 0.0, -1000.0), 0.0)
        coef[s, :, 3 * nodes : 4 * nodes] = dead.astype(jnp.bfloat16)
        at = lax.broadcasted_iota(jnp.int32, (cfg, 128), 0).astype(jnp.float32)
        pull[s] = shift * (HORIZON / nodes) - (at + 1.0) * step
        flat = lax.broadcasted_iota(jnp.int32, (nodes, cfg), 1).astype(jnp.float32)
        left = jnp.clip((flat + 1.0) * step - shift * (HORIZON / nodes), HORIZON / nodes, HORIZON)
        tenors = (lax.broadcasted_iota(jnp.int32, (nodes, cfg), 0).astype(jnp.float32) + 1.0) * (HORIZON / nodes)
        grid[s] = jnp.maximum(0.0, 1.0 - jnp.abs(left - tenors) * (nodes / HORIZON)).astype(jnp.bfloat16)
        line = lax.broadcasted_iota(jnp.int32, (dates, half), 0) == date
        row = jnp.where(x == 0, weight_ref[:, :half], weight_ref[:, half:])
        row = jnp.sum(jnp.where(line, row, 0.0), axis=0, keepdims=True) / total_paths * 0.5
        column[s] = jnp.transpose(jnp.broadcast_to(row, (128, half)))

    def discount(g, s):
        curve = curves[g, s]
        lines = jnp.concatenate([curve, curve, curve, jnp.ones(curve.shape, jnp.bfloat16)], axis=0)
        for m in range(0, cfg, 256):
            power = jnp.dot(coef[s, m : m + 256, :], lines, preferred_element_type=jnp.float32)
            target = pl.ds(pl.multiple_of(g * cfg + m, 256), 256)
            disc[s, target, :] = jnp.exp2(power).astype(jnp.bfloat16)

    stretch = cfg // 2
    fresh = [True] * slots

    def accumulate(g, side, s, level=None):
        extent = stretch if level is None else 2 * rows
        base = side * stretch + (0 if level is None else level // 2 * extent)
        at = pl.ds(pl.multiple_of(base, 16), extent)
        down = pl.ds(pl.multiple_of(g * cfg + base, 16), extent)
        product = lax.dot_general(
            cash[g, at, :], disc[s, down, :], (((0,), (0,)), ((), ())), preferred_element_type=jnp.float32
        )
        if fresh[s]:
            value[s] = product
        else:
            value[s] = value[s] + product
        fresh[s] = False

    group = (c, across, sibling, diagonal)

    def relayed(which):
        jump[which].wait_recv()
        there = block(group[which], far_level, y)
        relay[which] = remote(there, there, above)
        leave(which, far_level, there)

    def reached(which, copies, level):
        copies[which].wait_recv()
        leave(which, level, block(group[which], level, y))

    def shared(which, count):
        for level, copy in sides[which][:count]:
            copy.wait_recv()
            there = block(group[which], level, 1 - y)
            given[2 + which].append(remote(there, there, core))
        del sides[which][:count]

    def landed(which, count=None):
        for copy in given[which][:count]:
            copy.wait_recv()
        del given[which][:count]

    def priced(name, which, s):
        for copy in arriving[name, s]:
            copy.wait_recv()
        discount(group[which], s)

    keep.wait()
    for s in range(slots):
        discount(c, s)
    crossing.wait_recv()
    got = block(across, z, y)
    jump[1], hop[1] = remote(got, got, beyond), remote(got, got, above)
    leave(1, z, got)
    priced("sibling", 2, 0)
    relayed(0)
    for s in range(1, slots):
        priced("sibling", 2, s)
    reached(0, hop, next_level)
    shared(0, 1)
    priced("across", 1, 0)
    relayed(1)
    reached(0, relay, last_level)
    accumulate(c, y, 0)
    reached(1, hop, next_level)
    shared(0, 1)
    for s in range(1, slots):
        accumulate(c, y, s)
    shared(0, 1)
    landed(0)
    accumulate(sibling, y, 0)
    reached(1, relay, last_level)
    for s in range(1, slots):
        accumulate(sibling, y, s)
    shared(1, 1)
    accumulate(across, y, 0)
    priced("diagonal", 3, 0)
    shared(0, levels)
    accumulate(c, 1 - y, 0)
    shared(1, 1)
    for s in range(1, slots):
        accumulate(c, 1 - y, s)
        priced("across", 1, s)
        accumulate(across, y, s)
    shared(1, 1)
    landed(1)
    accumulate(diagonal, y, 0)
    landed(2)
    for s in range(slots):
        accumulate(sibling, 1 - y, s)
    shared(1, 1)
    for s in range(slots):
        accumulate(across, 1 - y, s, z)
    for s in range(1, slots):
        priced("diagonal", 3, s)
        accumulate(diagonal, y, s)
    shared(1, levels)
    landed(3, 3)
    for s in range(slots):
        accumulate(diagonal, 1 - y, s, z)
    for s in range(slots):
        accumulate(across, 1 - y, s, far_level)
    landed(3)
    for s in range(slots):
        accumulate(diagonal, 1 - y, s, far_level)

    part_s[...] = jnp.zeros(part_s.shape, jnp.float32)
    for s in range(slots):
        gained = jnp.zeros((half, 128), jnp.float32)
        for tile in range(paths // 128):
            cols = slice(tile * 128, tile * 128 + 128)
            held_value = value[s, :, cols]
            square = held_value * held_value + SOFTEN
            inverse = lax.rsqrt(square)
            gained = gained + 0.5 * (held_value + square * inverse)
            steep = column[s] * (1.0 + held_value * inverse)
            slope[s, cols, :] = jnp.transpose(steep).astype(jnp.bfloat16)
        gained = jnp.sum(jnp.transpose(gained), axis=0, keepdims=True) / total_paths
        for n in range(2):
            part_e[n, s] = gained[:, n * 128 : n * 128 + 128]

    twins = [((k + dk) % 2, (p + dp) % members) for dk in range(2) for dp in range(members)][1:]
    sums = [remote(part_e.at[n], held_e.at[k, p], (2 * x + n, q)) for n, q in twins]
    held_e[k, p] = part_e[k]
    for s in range(slots):
        for g in range(groups):
            for m in range(0, cfg, 256):
                down = pl.ds(g * cfg + m, 256)
                pulled = jnp.dot(disc[s, down, :], slope[s], preferred_element_type=jnp.float32)
                pulled = pulled * cash[g, m : m + 256, :].astype(jnp.float32)
                summed[g, m : m + 256, :] = (pulled[:, :128] + pulled[:, 128:]) * pull[s, m : m + 256, :]
            whole = summed[g]
            high = whole.astype(jnp.bfloat16)
            rest = (whole - high.astype(jnp.float32)).astype(jnp.bfloat16)
            pair = jnp.dot(
                grid[s], jnp.concatenate([high, rest], axis=1), preferred_element_type=jnp.float32
            )
            spread = jnp.transpose(pair[:, :128] + pair[:, 128:])
            part_s[s, g, :, :nodes] = jnp.sum(spread, axis=0, keepdims=True)
        sums += [remote(part_s.at[s, g], held_s.at[s, c, p], (g, q)) for g, q in others]
        held_s[s, c, p] = part_s[s, c]
    for copy in sums[: len(twins)]:
        copy.wait_recv()
    for d in range(dates):
        slot = date_ref[d]
        exp_ref[d : d + 1, :] = held_e[0, slot // slots, slot % slots] + held_e[1, slot // slots, slot % slots]
    for copy in sums[len(twins) :]:
        copy.wait_recv()
    for d in range(dates):
        slot = date_ref[d]
        q = slot // slots
        s = slot % slots
        total = held_s[s, 0, q]
        for g in range(1, groups):
            total = total + held_s[s, g, q]
        sens_ref[d : d + 1, :] = total[:, :nodes]
    for copy in started:
        copy.wait_send()


def settle_kernel(exposure_ref, sens_ref, exposure_out, sens_out, done):
    copies = [
        pltpu.make_async_copy(exposure_ref, exposure_out, done.at[0]),
        pltpu.make_async_copy(sens_ref, sens_out, done.at[1]),
    ]
    for copy in copies:
        copy.start()
    for copy in copies:
        copy.wait()


def by_slot(curve_store, cash_index, cash_amount, trade_set, date_slot, default_weight):
    groups, members = lax.axis_size("ccy"), lax.axis_size("path")
    _, slots, nodes, total_paths = curve_store.shape
    trades, flows = cash_index.shape[1:]
    dates, nsets = default_weight.shape
    rows, half, paths = CFG // members, nsets // 2, total_paths // 2
    levels = members // 2
    count = 1 + 6 + 2 * levels + 4 * levels + 3 * slots + 2 * members - 1 + slots * (groups * members - 1)
    vmem = pl.BlockSpec(memory_space=pltpu.VMEM)
    bf16, f32 = jnp.bfloat16, jnp.float32
    operands = (date_slot, cash_index[0].T, cash_amount[0].T, trade_set, default_weight, curve_store[0])
    exposure, sens = pl.pallas_call(
        functools.partial(fused_kernel, total_paths),
        out_shape=[
            jax.ShapeDtypeStruct((dates, nsets // groups), f32),
            jax.ShapeDtypeStruct((dates, nodes), f32),
        ],
        in_specs=[pl.BlockSpec(memory_space=pltpu.HBM)] * 6,
        out_specs=[vmem, vmem],
        scratch_shapes=[
            pltpu.SMEM((dates,), jnp.int32),
            pltpu.VMEM((flows, trades), jnp.int32),
            pltpu.VMEM((flows, trades), f32),
            pltpu.VMEM((1, trades), jnp.int32),
            pltpu.VMEM((dates, nsets), f32),
            pltpu.VMEM((2 * rows, trades), bf16),
            pltpu.VMEM((nsets, trades), bf16),
            pltpu.VMEM((groups, CFG, half), bf16),
            pltpu.VMEM((rows, half), bf16),
            pltpu.VMEM((groups, slots, nodes, paths), bf16),
            pltpu.VMEM((slots, CFG, 4 * nodes), bf16),
            pltpu.VMEM((slots, CFG, 128), f32),
            pltpu.VMEM((slots, nodes, CFG), bf16),
            pltpu.VMEM((slots, half, 128), f32),
            pltpu.VMEM((slots, groups * CFG, paths), bf16),
            pltpu.VMEM((slots, half, paths), f32),
            pltpu.VMEM((slots, paths, half), bf16),
            pltpu.VMEM((groups, CFG, 128), f32),
            pltpu.VMEM((2, slots, 1, 128), f32),
            pltpu.VMEM((slots, groups, 1, 128), f32),
            pltpu.VMEM((2, members, slots, 1, 128), f32),
            pltpu.VMEM((slots, groups, members, 1, 128), f32),
            pltpu.SemaphoreType.DMA((count,)),
            pltpu.SemaphoreType.DMA((count,)),
            pltpu.SemaphoreType.DMA((6,)),
        ],
        compiler_params=pltpu.CompilerParams(
            collective_id=0, has_side_effects=True, vmem_limit_bytes=48 * 1024 * 1024
        ),
        name="fused",
    )(*(pltpu.with_memory_space_constraint(operand, pltpu.HBM) for operand in operands))
    exposure, sens = pl.pallas_call(
        settle_kernel,
        out_shape=[jax.ShapeDtypeStruct(array.shape, array.dtype) for array in (exposure, sens)],
        in_specs=[vmem, vmem],
        out_specs=[pl.BlockSpec(memory_space=pltpu.HBM)] * 2,
        scratch_shapes=[pltpu.SemaphoreType.DMA((2,))],
        compiler_params=pltpu.CompilerParams(vmem_limit_bytes=1024 * 1024),
        name="settle",
    )(exposure, sens)
    return (exposure, sens[None])


def by_path(curve_store, cash_index, cash_amount, trade_set, date_slot, default_weight):
    groups = lax.axis_size("ccy")
    group_index = lax.axis_index("ccy")
    members = lax.axis_size("path")
    nodes, total_paths = curve_store.shape[2], curve_store.shape[3]
    nsets = default_weight.shape[1]
    share_size = nsets // groups
    rows = CFG // members
    base = (lax.axis_index("path") * rows).astype(jnp.int32)[None]
    chunk = build_cash(base, cash_index[0], cash_amount[0], trade_set[0], rows, nsets)
    cash_table = lax.all_gather(chunk, "path", axis=0, tiled=True)
    blocks = lax.all_to_all(curve_store, "path", split_axis=3, concat_axis=1, tiled=True)[0]
    cash_all = lax.all_gather(cash_table[None], "ccy", axis=0, tiled=True)

    def advance(unused, inputs):
        date_index, slot_id, weight_row = inputs
        remain, alive_mask, weights = date_tables(date_index, nodes, CFG)
        grid_weights = weights.astype(jnp.bfloat16)
        curve_now = lax.dynamic_index_in_dim(blocks, slot_id, 0, keepdims=False)
        curve_groups = lax.all_gather(curve_now[None], "ccy", axis=0, tiled=True)
        yields = jnp.einsum(
            "gnp,nc->gpc", curve_groups, grid_weights, preferred_element_type=jnp.float32
        )
        discount_all = alive_mask * jnp.exp(-yields * remain)
        values = jnp.einsum(
            "gpc,gcs->ps", discount_all.astype(jnp.bfloat16), cash_all,
            preferred_element_type=jnp.float32,
        )
        discount = lax.dynamic_index_in_dim(discount_all, group_index, 0, keepdims=False)
        rooted = jnp.sqrt(values * values + SOFTEN)
        slopes = (weight_row / total_paths * 0.5 * (1.0 + values / rooted)).astype(jnp.bfloat16)
        share_values = lax.dynamic_slice_in_dim(values, group_index * share_size, share_size, 1)
        share_root = lax.dynamic_slice_in_dim(rooted, group_index * share_size, share_size, 1)
        exposure_part = jnp.sum(0.5 * (share_values + share_root), axis=0) / total_paths
        back_flow = lax.dot_general(
            slopes, cash_table, (((1,), (1,)), ((), ())), preferred_element_type=jnp.float32
        )
        node_pull = jnp.sum(back_flow * -remain * discount, axis=0)
        sens_part = jnp.dot(weights, node_pull, precision=lax.Precision.HIGHEST)
        exposure_part, sens_part = lax.psum((exposure_part, sens_part), "path")
        return (unused, (exposure_part, sens_part))

    inputs = (jnp.arange(date_slot.shape[0], dtype=jnp.int32), date_slot, default_weight)
    _, (exposure_rows, sens_rows) = lax.scan(advance, jnp.zeros((), jnp.float32), inputs)
    return (exposure_rows, sens_rows[None])


def local(curve_store, cash_index, cash_amount, trade_set, date_slot, default_weight):
    groups, members = lax.axis_size("ccy"), lax.axis_size("path")
    slots, nodes, total_paths = curve_store.shape[1:]
    nsets = default_weight.shape[1]
    trades = trade_set.shape[1]
    fits = groups == 4 and members == 8 and slots * members == date_slot.shape[0]
    fits = fits and nodes * 0.5 == HORIZON and CFG == 16 * nodes and total_paths % 256 == 0
    fits = fits and nsets == 4 * 128 and CFG // members == 128 and trades % 128 == 0
    plan = by_slot if fits else by_path
    return plan(curve_store, cash_index, cash_amount, trade_set, date_slot, default_weight)


def solution(mesh):
    in_specs = (
        P("ccy", "path", None, None),
        P("ccy", None, None),
        P("ccy", None, None),
        P("ccy", None),
        P(),
        P(),
    )
    out_specs = (P(None, "ccy"), P("ccy", None, None))
    return jax.shard_map(local, mesh=mesh, in_specs=in_specs, out_specs=out_specs, check_vma=False)
```
